32 devices in a mesh: gx: 4 (over z), gy: 4 (over y, x), gz: 2 (over core).
Axes of the slice: x: 2, y: 2, z: 4, core: 2. Of those that a mesh axis runs over, the one named last changes fastest.
Arguments:
- velocity: float32 [3, 32, 64, 256], P(None, 'gx', 'gy', 'gz'), may hold values from -6 to 6
- density: float32 [32, 64, 256], P('gx', 'gy', 'gz'), may hold values from 0 to 2
- offsets: int32 [3, 32, 64, 256], P(None, 'gx', 'gy', 'gz'), may hold values from -4 to 3
- eighths: int32 [3, 32, 64, 256], P(None, 'gx', 'gy', 'gz'), may hold values from 0 to 7
Outputs:
- new_velocity: float32 [3, 32, 64, 256], P(None, 'gx', 'gy', 'gz')
- new_density: float32 [32, 64, 256], P('gx', 'gy', 'gz')
- pressure: float32 [32, 64, 256], P('gx', 'gy', 'gz')
The draws below stay inside these ranges and needn't reach their ends.
All inputs are finite; a program needn't handle non-finite values.
Results may differ from the reference program's by a relative error of at most 0.00002.
Values sent between devices are 32-bit elements; how exact they have to be, the bound alone decides.
A program may use at most 64 MiB of HBM per device.

```python
import jax
import jax.numpy as jnp
from jax import lax

NX = 32
NY = 64
NZ = 256


def set_ends(values, key, low, high):
    index_at = [jax.random.randint(jax.random.fold_in(key, axis), (), 0, length) for axis, length in enumerate(values.shape)]
    main_axis = values.shape.index(max(values.shape))
    next_to = index_at[:main_axis] + [(index_at[main_axis] + 1) % values.shape[main_axis]] + index_at[main_axis + 1:]
    return values.at[tuple(index_at)].set(low).at[tuple(next_to)].set(high)


def block_levels(key, dims, split, smallest, top_value):
    def one(dim, blocks):
        steps = jax.random.uniform(jax.random.fold_in(jax.random.fold_in(key, 6), dim), (blocks,), jnp.float32, smallest / len(split), top_value / len(split))
        return jnp.repeat(jnp.exp(steps), dims[dim] // blocks).reshape((-1,) + (1,) * (len(dims) - dim - 1))

    level = one(*split[0])
    for cut in split[1:]:
        level = level * one(*cut)
    return level


def noise(own_key, shape, width, limit, shards=(), held_as=jnp.bfloat16):
    gain = block_levels(own_key, shape, shards, -0.22, 0.18) if shards else 1.0
    array = jax.random.normal(own_key, shape, jnp.float32) * width * gain
    return jnp.minimum(jnp.maximum(array, -limit), limit).astype(held_as)


def setup_inputs(seed: int = 0) -> dict:
    key_list = jax.random.split(jax.random.key(seed), 5)
    velocity = noise(key_list[0], (3, NX, NY, NZ), 1.0, 6.0, ((1, 4), (2, 4), (3, 2)), jnp.float32)
    density = jnp.clip(2.0 * jax.random.uniform(key_list[1], (NX, NY, NZ), jnp.float32) ** block_levels(key_list[1], (NX, NY, NZ), ((0, 4), (1, 4), (2, 2)), -0.2, 0.2), 0.0, 2.0)
    offsets = set_ends(jax.random.randint(key_list[2], (3, NX, NY, NZ), -4, 4), jax.random.fold_in(key_list[2], 1), -4, 3).astype(jnp.int32)
    eighths = set_ends(jax.random.randint(key_list[3], (3, NX, NY, NZ), 0, 8), jax.random.fold_in(key_list[3], 1), 0, 7).astype(jnp.int32)
    return dict(velocity=velocity, density=density, offsets=offsets, eighths=eighths)


RELAX_WEIGHT = 6.0 / 7.0


def neighbours(padded):
    summed = padded[2:, 1:-1, 1:-1] + padded[:-2, 1:-1, 1:-1]
    summed = summed + padded[1:-1, 2:, 1:-1] + padded[1:-1, :-2, 1:-1]
    summed = summed + padded[1:-1, 1:-1, 2:] + padded[1:-1, 1:-1, :-2]
    return summed


def operate(padded):
    return 6.0 * padded[1:-1, 1:-1, 1:-1] - neighbours(padded)


def advect_block(padded, offsets, eighths):
    field_count = padded.shape[0]
    stride_y = padded.shape[3]
    stride_x = padded.shape[2] * padded.shape[3]
    flattened = padded.reshape(field_count, -1)
    box_shape = offsets.shape[1:]
    base_x = lax.broadcasted_iota(jnp.int32, box_shape, 0) + 4 + offsets[0]
    base_y = lax.broadcasted_iota(jnp.int32, box_shape, 1) + 4 + offsets[1]
    base_z = lax.broadcasted_iota(jnp.int32, box_shape, 2) + 4 + offsets[2]
    fraction = eighths.astype(jnp.float32) / 8.0
    summed = jnp.zeros((field_count,) + box_shape, jnp.float32)
    for shift_x in (0, 1):
        weight_x = fraction[0] if shift_x else 1.0 - fraction[0]
        for shift_y in (0, 1):
            weight_y = fraction[1] if shift_y else 1.0 - fraction[1]
            for shift_z in (0, 1):
                weight_z = fraction[2] if shift_z else 1.0 - fraction[2]
                weight = weight_x * weight_y * weight_z
                position = (base_x + shift_x) * stride_x + (base_y + shift_y) * stride_y + base_z + shift_z
                picked = jnp.take(flattened, position.reshape(-1), axis=1).reshape(summed.shape)
                summed = summed + weight[None] * picked
    return summed


def divergence_of(velocity_pad):
    part_x = velocity_pad[0, 2:, 1:-1, 1:-1] - velocity_pad[0, :-2, 1:-1, 1:-1]
    part_y = velocity_pad[1, 1:-1, 2:, 1:-1] - velocity_pad[1, 1:-1, :-2, 1:-1]
    part_z = velocity_pad[2, 1:-1, 1:-1, 2:] - velocity_pad[2, 1:-1, 1:-1, :-2]
    return 0.5 * (part_x + part_y + part_z)


def gradient_of(pressure_pad):
    part_x = pressure_pad[2:, 1:-1, 1:-1] - pressure_pad[:-2, 1:-1, 1:-1]
    part_y = pressure_pad[1:-1, 2:, 1:-1] - pressure_pad[1:-1, :-2, 1:-1]
    part_z = pressure_pad[1:-1, 1:-1, 2:] - pressure_pad[1:-1, 1:-1, :-2]
    return 0.5 * jnp.stack([part_x, part_y, part_z], axis=0)


def restrict(field):
    return field.reshape(field.shape[0] // 2, 2, field.shape[1] // 2, 2, field.shape[2] // 2, 2).mean(axis=(1, 3, 5))


def prolong(field):
    return jnp.repeat(jnp.repeat(jnp.repeat(field, 2, axis=0), 2, axis=1), 2, axis=2)


def sweeps(source, spacing):
    relaxation = RELAX_WEIGHT / 6.0
    first_sweep = relaxation * spacing * source
    second_sweep = first_sweep + relaxation * (spacing * source - operate(jnp.pad(first_sweep, 1)))
    return second_sweep


def smooth_level(source, spacing):
    second_sweep = sweeps(source, spacing)
    residual = source - operate(jnp.pad(second_sweep, 1)) / spacing
    return second_sweep, residual


def reference(velocity, density, offsets, eighths):
    fields = jnp.concatenate([velocity, density[None]], axis=0)
    padded = jnp.pad(fields, ((0, 0), (4, 4), (4, 4), (4, 4)))
    advected = advect_block(padded, offsets, eighths)
    velocity_pad = jnp.pad(advected[:3], ((0, 0), (1, 1), (1, 1), (1, 1)))
    divergence = divergence_of(velocity_pad)
    fine_sweep, fine_residual = smooth_level(-divergence, 1.0)
    middle_sweep, middle_residual = smooth_level(restrict(fine_residual), 4.0)
    coarse_sweep = sweeps(restrict(middle_residual), 16.0)
    pressure = fine_sweep + prolong(middle_sweep + prolong(coarse_sweep))
    gradient = gradient_of(jnp.pad(pressure, 1))
    return advected[:3] - gradient, advected[3], pressure
```

```python
import functools

import jax
import jax.numpy as jnp
from jax import lax
from jax.experimental import pallas as pl
from jax.experimental.pallas import tpu as pltpu
from jax.sharding import PartitionSpec as P

MESH = pl.DeviceIdType.MESH
RELAX = (6.0 / 7.0) / 6.0
HALO = 4
XY = [(dx, dy) for dx in (-1, 0, 1) for dy in (-1, 0, 1) if (dx, dy) != (0, 0)]


def lanes(shape):
    return lax.broadcasted_iota(jnp.int32, shape, len(shape) - 1)


def roll(x, shift, axis):
    shift = shift % x.shape[axis]
    return x if shift == 0 else pltpu.roll(x, shift, axis)


def inside(sizes, me, delta):
    ok = None
    for n, i, d in zip(sizes, me, delta):
        if d:
            one = (i + d >= 0) & (i + d < n)
            ok = one if ok is None else ok & one
    return ok


class Comm:
    def __init__(self, sizes, me, send, recv):
        self.sizes, self.me, self.send, self.recv = sizes, me, send, recv
        self.copies = []

    def add(self, delta, src, dst, slot):
        device = tuple(i + d for i, d in zip(self.me, delta))
        copy = pltpu.make_async_remote_copy(
            src_ref=src, dst_ref=dst, send_sem=self.send.at[slot], recv_sem=self.recv.at[slot],
            device_id=device, device_id_type=MESH,
        )
        to = inside(self.sizes, self.me, delta)
        source = inside(self.sizes, self.me, tuple(-d for d in delta))
        pl.when(to)(copy.start)
        self.copies.append((copy, to, source))

    def wait(self):
        for copy, to, source in self.copies:
            pl.when(source)(copy.wait_recv)
        for copy, to, source in self.copies:
            pl.when(to)(copy.wait_send)


def zero_if_missing(sizes, me, delta, ref):
    @pl.when(jnp.logical_not(inside(sizes, me, delta)))
    def _():
        ref[...] = jnp.zeros(ref.shape, ref.dtype)


def pick_x(d):
    return {-1: 0, 1: 1}[d]


def exchange_xy(sizes, me, own, strips, rx, ry, rc, sems, out, meanwhile=None):
    f, p, r, _ = own.shape
    hx, hy = rx.shape[2], ry.shape[3]
    for i in range(p):
        strips[0, :, i] = own[:, i, 0:hy, :]
        strips[1, :, i] = own[:, i, r - hy : r, :]
    comm = Comm(sizes, me, *sems)
    for slot, (dx, dy) in enumerate(XY):
        xs = slice(0, hx) if dx < 0 else slice(p - hx, p)
        if dy == 0:
            src, dst = own.at[:, xs], rx.at[pick_x(-dx)]
        elif dx == 0:
            src, dst = strips.at[pick_x(dy)], ry.at[pick_x(-dy)]
        else:
            src, dst = strips.at[pick_x(dy), :, xs], rc.at[pick_x(-dx), pick_x(-dy)]
        comm.add((dx, dy, 0), src, dst, slot)
    for dx, dy in XY:
        ref = rx.at[pick_x(dx)] if dy == 0 else ry.at[pick_x(dy)] if dx == 0 else rc.at[pick_x(dx), pick_x(dy)]
        zero_if_missing(sizes, me, (dx, dy, 0), ref)
    out[:, HALO : HALO + p, HALO : HALO + r, :] = own[...]
    if meanwhile is not None:
        meanwhile()
    comm.wait()
    for sx, xs in ((0, slice(HALO - hx, HALO)), (1, slice(HALO + p, HALO + p + hx))):
        out[:, xs, HALO : HALO + r, :] = rx[sx]
        for sy, ys in ((0, slice(HALO - hy, HALO)), (1, slice(HALO + r, HALO + r + hy))):
            out[:, xs, ys, :] = rc[sx, sy]
    for sy, ys in ((0, slice(HALO - hy, HALO)), (1, slice(HALO + r, HALO + r + hy))):
        out[:, HALO : HALO + p, ys, :] = ry[sy]


class ZExchange:
    def __init__(self, sizes, me, own, got, sems):
        self.comm = Comm(sizes, me, *sems)
        self.comm.add((0, 0, -1), own, got.at[1], 0)
        self.comm.add((0, 0, 1), own, got.at[0], 1)
        zero_if_missing(sizes, me, (0, 0, -1), got.at[0])
        zero_if_missing(sizes, me, (0, 0, 1), got.at[1])
        self.wait = self.comm.wait


def swap_blocks(regs, width, shift=0):
    n = len(regs)
    lane = lanes(regs[0].shape)
    into, outof = ((lane + shift) & 127) // width, lane // width
    bits = [1 << k for k in range(n.bit_length() - 1)]
    for bit in bits:
        mask = (into & bit) != 0
        regs = [jnp.where(mask, regs[(i + bit) % n], regs[i]) for i in range(n)]
    regs = [roll(regs[i], width * i + shift, 1) for i in range(n)]
    regs = [regs[-i % n] for i in range(n)]
    for bit in bits:
        mask = (outof & bit) != 0
        regs = [jnp.where(mask, regs[(i - bit) % n], regs[i]) for i in range(n)]
    return regs


def pack_z(ext, packed):
    f, p, rows, _ = ext.shape
    lane = lanes((rows, 128))
    for c in range(f):
        total = roll(ext[c, 0], 4, 1)
        for x in range(1, p):
            total = jnp.where(lane >= 8 * x, roll(ext[c, x], 4 + 8 * x, 1), total)
        packed[c] = total


def gather(x, index):
    return jnp.take_along_axis(x, index, axis=1, mode="promise_in_bounds")


def advect_pair(code, load):
    lane = lanes((8, 128))
    part = (lane >> 3) & 1
    first = part == 0
    sums = []
    for half in range(2):
        v = jnp.where(first, code, roll(code, 8, 1)) if half == 0 else jnp.where(first, roll(code, -8, 1), code)
        ox, oy, oz = v & 7, (v >> 3) & 7, (v >> 6) & 7
        fx = ((v >> 9) & 7).astype(jnp.float32) * 0.125
        fy = ((v >> 12) & 7).astype(jnp.float32) * 0.125
        fz = ((v >> 15) & 7).astype(jnp.float32) * 0.125
        spot = (lane & 7) + oz + part
        near = spot < 8
        index = [((lane >> 4) + ox + cx) * 8 + (spot & 7) for cx in range(2)]
        wz = jnp.where(first, 1.0 - fz, fz)
        totals = [[None] * 2 for _ in range(4)]
        for dy in range(9):
            if dy == 0:
                wy = jnp.where(oy == 0, 1.0 - fy, 0.0)
            elif dy == 8:
                wy = jnp.where(oy == 7, fy, 0.0)
            else:
                wy = jnp.where(oy == dy, 1.0 - fy, jnp.where(oy == dy - 1, fy, 0.0))
            for c in range(4):
                one, two = load(c, half, dy), load(c, half + 1, dy)
                for cx in range(2):
                    value = wy * jnp.where(near, gather(one, index[cx]), gather(two, index[cx]))
                    totals[c][cx] = value if dy == 0 else totals[c][cx] + value
        wx0, wx1 = (1.0 - fx) * wz, fx * wz
        sums.append([wx0 * totals[c][0] + wx1 * totals[c][1] for c in range(4)])
    out = []
    for c in range(4):
        keep = jnp.where(first, sums[0][c], sums[1][c])
        move = jnp.where(first, sums[1][c], sums[0][c])
        out.append(keep + jnp.where(first, roll(move, -8, 1), roll(move, 8, 1)))
    return out


def kernel(sizes, vel_hbm, den_hbm, off_hbm, eig_hbm, new_vel, new_den, press, off, eig, fetch_sem, fields, stripA, rxA, ryA, rcA, ext,
           edge, gotP, src, code, codeT, resT, u, stripB, rxB, ryB, rcB, extU, packU, gotU, wide, s0, q0, r0,
           tmp0, own1, strip1, rx1, ry1, rc1, ext1, got1, wide1, q1, r1, tmp1, own2, got2, ext2, gotz2, sum1, fine,
           sxyA, rxyA, szA, rzA, sxyB, rxyB, szB, rzB, sxy1, rxy1, sz1, rz1, sxy2, rxy2, sz2, rz2):
    me = tuple(lax.axis_index(a) for a in ("gx", "gy", "gz"))
    p, r = fields.shape[1], fields.shape[2]
    pairs = [(vel_hbm, fields.at[0:3]), (den_hbm, fields.at[3]), (off_hbm, off), (eig_hbm, eig)]
    fetch = [pltpu.make_async_copy(a, b, fetch_sem.at[i]) for i, (a, b) in enumerate(pairs)]
    for copy in fetch:
        copy.start()

    barrier = pltpu.get_barrier_semaphore()
    peers = [(dx, dy, 0) for dx, dy in XY] + [(0, 0, -1), (0, 0, 1)]
    count = jnp.int32(0)
    for delta in peers:
        ok = inside(sizes, me, delta)

        @pl.when(ok)
        def _():
            pl.semaphore_signal(barrier, inc=1, device_id=tuple(i + d for i, d in zip(me, delta)), device_id_type=MESH)

        count = count + jnp.where(ok, 1, 0)
    for copy in fetch[:2]:
        copy.wait()
    pl.semaphore_wait(barrier, count)

    def positions():
        for copy in fetch[2:]:
            copy.wait()
        whole = (off[0] + 4) + 8 * (off[1] + 4) + 64 * (off[2] + 4)
        code[...] = whole + 512 * eig[0] + 4096 * eig[1] + 32768 * eig[2]
        for t in range(r // 8):
            for q, v in enumerate(swap_blocks([code[x, 8 * t : 8 * t + 8] for x in range(p)], 16)):
                codeT[t, q] = v

    exchange_xy(sizes, me, fields, stripA, rxA, ryA, rcA, (sxyA, rxyA), ext, positions)

    rows = r + 8
    tiles = rows // 8
    blocks = 128 // 8
    lane16 = lanes((r, 128))
    lane = lanes((rows, 128))

    def turn(c, carry):
        for t in range(tiles):
            for b, v in enumerate(swap_blocks([ext[c, x, 8 * t : 8 * t + 8] for x in range(p + 8)], 8, 4)):
                if b == 0:
                    edge[c, 8 * t : 8 * t + 8] = v
                else:
                    src[c, b, 8 * t : 8 * t + 8] = v
        return carry

    lax.fori_loop(0, 4, turn, 0)
    zA = ZExchange(sizes, me, edge, gotP, (szA, rzA))

    def advect(t, q):
        totals = advect_pair(codeT[t, q], lambda c, b, dy: src[c, 2 * q + b, 8 * t + dy : 8 * t + dy + 8, :])
        for c in range(4):
            resT[c, t, q] = totals[c]

    def middle(q, carry):
        for t in range(r // 8):
            advect(t, q)
        return carry

    lax.fori_loop(1, blocks // 2 - 1, middle, 0)
    zA.wait()
    low = (lane & 7) < 4
    for c in range(4):
        src[c, 0] = jnp.where(low, gotP[0, c], edge[c])
        src[c, blocks] = jnp.where(low, edge[c], gotP[1, c])

    def ends(i, carry):
        for t in range(r // 8):
            advect(t, i * (blocks // 2 - 1))
        return carry

    lax.fori_loop(0, 2, ends, 0)

    def back(c, carry):
        for t in range(r // 8):
            for x, v in enumerate(swap_blocks([resT[c, t, q] for q in range(blocks // 2)], 16)):
                u[c, x, 8 * t : 8 * t + 8] = v
        return carry

    lax.fori_loop(0, 4, back, 0)
    new_den[...] = u[3]

    vel_u = u.at[0:3]
    exchange_xy(sizes, me, vel_u, stripB, rxB, ryB, rcB, (sxyB, rxyB), extU)
    pack_z(extU, packU)
    ZExchange(sizes, me, packU, gotU, (szB, rzB)).wait()
    for c in range(3):
        both = jnp.where((lane & 7) < 4, gotU[0, c], gotU[1, c])
        for x in range(HALO - 3, HALO + p + 3):
            wide[c, x, :, 0:128] = extU[c, x]
            wide[c, x, :, 128:256] = roll(both, -(8 * x + 4), 1)

    def yz_mask(nrows, first_row, block_rows, cells):
        row = lax.broadcasted_iota(jnp.int32, (nrows, 256), 0) - first_row + me[1] * block_rows
        spot = lanes((nrows, 256))
        z = jnp.where(spot < 192, spot, spot - 256) + me[2] * cells
        return (row >= 0) & (row < sizes[1] * block_rows) & (z >= 0) & (z < sizes[2] * cells)

    def x_ok(x, first, block):
        g = x - first + me[0] * block
        return (g >= 0) & (g < sizes[0] * block)

    mask0 = yz_mask(rows, HALO, r, 128)

    def around(ref, x, step):
        v = ref[x]
        total = ref[x + 1] + ref[x - 1]
        total = total + roll(v, -1, 0) + roll(v, 1, 0)
        total = total + roll(v, -step, 1) + roll(v, step, 1)
        return 6.0 * v - total

    def second(ref, x, scale, step):
        v = ref[x]
        first = (RELAX * scale) * v
        return first + RELAX * (scale * v - (RELAX * scale) * around(ref, x, step))

    def source0(x, carry):
        part = wide[0, x + 1] - wide[0, x - 1]
        v = wide[1, x]
        part = part + (roll(v, -1, 0) - roll(v, 1, 0))
        v = wide[2, x]
        part = part + (roll(v, -1, 1) - roll(v, 1, 1))
        s0[x] = jnp.where(mask0 & x_ok(x, HALO, p), -0.5 * part, 0.0)
        return carry

    lax.fori_loop(HALO - 2, HALO + p + 2, source0, 0)

    def second0(x, carry):
        q0[x] = jnp.where(mask0 & x_ok(x, HALO, p), second(s0, x, 1.0, 1), 0.0)
        return carry

    lax.fori_loop(HALO - 1, HALO + p + 1, second0, 0)

    def residual0(x, carry):
        r0[x] = (s0[x] - around(q0, x, 1))[:, 0:128]
        return carry

    lax.fori_loop(HALO, HALO + p, residual0, 0)
    lane8 = lanes((r // 2, 128))
    for x in range(p // 2):
        tmp0[...] = r0[HALO + 2 * x] + r0[HALO + 2 * x + 1]
        v = tmp0[pl.ds(HALO, r // 2, stride=2), :] + tmp0[pl.ds(HALO + 1, r // 2, stride=2), :]
        v = v + jnp.where((lane8 & 1) == 0, roll(v, -1, 1), roll(v, 1, 1))
        own1[0, x] = 0.125 * v

    p1, r1n = p // 2, r // 2
    exchange_xy(sizes, me, own1, strip1, rx1, ry1, rc1, (sxy1, rxy1), ext1)
    near1 = pl.ds(HALO - 2, p1 + 4)
    ZExchange(sizes, me, ext1.at[0, near1], got1, (sz1, rz1)).wait()
    rows1 = r1n + 8
    lane1 = lanes((rows1, 128))
    for x in range(HALO - 2, HALO + p1 + 2):
        wide1[x, :, 0:128] = ext1[0, x]
        wide1[x, :, 128:256] = jnp.where(lane1 < 64, got1[1, x - HALO + 2], got1[0, x - HALO + 2])
    mask1 = yz_mask(rows1, HALO, r1n, 128)
    for x in range(HALO - 1, HALO + p1 + 1):
        q1[x] = jnp.where(mask1 & x_ok(x, HALO, p1), second(wide1, x, 4.0, 2), 0.0)
    for x in range(HALO, HALO + p1):
        r1[x] = (wide1[x] - 0.25 * around(q1, x, 2))[:, 0:128]
    p2, r2n = p1 // 2, r1n // 2
    lane4 = lanes((r2n, 128))
    for x in range(p2):
        tmp1[...] = r1[HALO + 2 * x] + r1[HALO + 2 * x + 1]
        v = tmp1[pl.ds(HALO, r2n, stride=2), :] + tmp1[pl.ds(HALO + 1, r2n, stride=2), :]
        v = v + jnp.where((lane4 & 3) < 2, roll(v, -2, 1), roll(v, 2, 1))
        own2[x] = 0.125 * v

    comm = Comm(sizes, me, sxy2, rxy2)
    for slot, (dx, dy) in enumerate(XY):
        comm.add((dx, dy, 0), own2, got2.at[1 - dx, 1 - dy], slot)
    for dx, dy in XY:
        zero_if_missing(sizes, me, (dx, dy, 0), got2.at[dx + 1, dy + 1])
    got2[1, 1] = own2[...]
    ext2[...] = jnp.zeros(ext2.shape, jnp.float32)
    comm.wait()
    for a in range(3):
        for b in range(3):
            ext2[p2 * a : p2 * a + p2, r2n * b : r2n * b + r2n, :] = got2[a, b]
    ZExchange(sizes, me, ext2, gotz2, (sz2, rz2)).wait()
    lane2 = lanes((16, 128))
    mask2 = yz_mask(16, r2n, r2n, 128)
    planes2 = {}
    for x in range(p2 - 2, 2 * p2 + 2):
        planes2[x] = jnp.concatenate([ext2[x], jnp.where(lane2 < 64, gotz2[1, x], gotz2[0, x])], axis=1)
    sum1[...] = jnp.zeros(sum1.shape, jnp.float32)
    for x in range(p2 - 1, 2 * p2 + 1):
        v = jnp.where(mask2 & x_ok(x, p2, p2), second(planes2, x, 16.0, 4), 0.0)
        first_row = r2n - 1
        take = r2n + 2
        base = HALO - 2
        for side in range(2):
            part = v[first_row : first_row + take, 128 * side : 128 * side + 128]
            sum1[x, side, pl.ds(base, take, stride=2), :] = part
            sum1[x, side, pl.ds(base + 1, take, stride=2), :] = part
    for x1 in range(HALO - 1, HALO + p1 + 1):
        x2 = (x1 - HALO) // 2 + p2
        for side in range(2):
            v = q1[x1, :, 128 * side : 128 * side + 128] + sum1[x2, side]
            part = v[HALO - 2 : HALO - 2 + r1n + 4]
            fine[x1, side, pl.ds(0, r1n + 4, stride=2), :] = part
            fine[x1, side, pl.ds(1, r1n + 4, stride=2), :] = part
    for x in range(HALO - 1, HALO + p + 1):
        x1 = (x - HALO) // 2 + HALO
        coarse = jnp.concatenate([fine[x1, 0], fine[x1, 1]], axis=1)
        s0[x] = jnp.where(mask0 & x_ok(x, HALO, p), q0[x] + coarse, 0.0)
    for x in range(p):
        v = s0[x + HALO]
        cut = lambda t: t[HALO : HALO + r, 0:128]
        press[x] = cut(v)
        new_vel[0, x] = u[0, x] - 0.5 * cut(s0[x + HALO + 1] - s0[x + HALO - 1])
        new_vel[1, x] = u[1, x] - 0.5 * cut(roll(v, -1, 0) - roll(v, 1, 0))
        new_vel[2, x] = u[2, x] - 0.5 * cut(roll(v, -1, 1) - roll(v, 1, 1))


def step(sizes, velocity, density, offsets, eighths):
    p, r, _ = density.shape
    f32 = jnp.float32

    def vm(*shape):
        return pltpu.VMEM(shape, f32)

    def xy(f, p, r, hx, hy):
        return [vm(2, f, p, hy, 128), vm(2, f, hx, r, 128), vm(2, f, p, hy, 128), vm(2, 2, f, hx, hy, 128)]

    assert p == 8 and r % 8 == 0
    p1, r1, p2, r2 = p // 2, r // 2, p // 4, r // 4
    rows, rows1 = r + 8, r1 + 8
    dma = lambda n: pltpu.SemaphoreType.DMA((n,))
    scratch = (
        [pltpu.VMEM(offsets.shape, jnp.int32), pltpu.VMEM(eighths.shape, jnp.int32), dma(4), vm(4, p, r, 128)] + xy(4, p, r, 4, 4)
        + [vm(4, p + 8, rows, 128), vm(4, rows, 128), vm(2, 4, rows, 128), vm(4, 17, rows, 128),
           pltpu.VMEM((p, r, 128), jnp.int32), pltpu.VMEM((r // 8, 8, 8, 128), jnp.int32),
           vm(4, r // 8, 8, 8, 128), vm(4, p, r, 128)]
        + xy(3, p, r, 3, 4)
        + [vm(3, p + 8, rows, 128), vm(3, rows, 128), vm(2, 3, rows, 128), vm(3, p + 8, rows, 256),
           vm(p + 8, rows, 256), vm(p + 8, rows, 256), vm(p + 8, rows, 128), vm(rows, 128), vm(1, p1, r1, 128)]
        + xy(1, p1, r1, 2, 2)
        + [vm(1, p1 + 8, rows1, 128), vm(2, p1 + 4, rows1, 128), vm(p1 + 8, rows1, 256), vm(p1 + 8, rows1, 256),
           vm(p1 + 8, rows1, 128), vm(rows1, 128), vm(p2, r2, 128), vm(3, 3, p2, r2, 128), vm(3 * p2, 16, 128),
           vm(2, 3 * p2, 16, 128), vm(3 * p2, 2, rows1, 128), vm(p1 + 8, 2, rows, 128)]
        + [dma(8), dma(8), dma(2), dma(2)] * 4
    )
    vmem = pl.BlockSpec(memory_space=pltpu.VMEM)
    return pl.pallas_call(
        functools.partial(kernel, sizes),
        out_shape=(
            jax.ShapeDtypeStruct(velocity.shape, f32),
            jax.ShapeDtypeStruct(density.shape, f32),
            jax.ShapeDtypeStruct(density.shape, f32),
        ),
        in_specs=[pl.BlockSpec(memory_space=pltpu.HBM)] * 4,
        out_specs=(vmem,) * 3,
        scratch_shapes=scratch,
        compiler_params=pltpu.CompilerParams(
            collective_id=0, has_side_effects=True, vmem_limit_bytes=60 * 1024 * 1024
        ),
    )(velocity, density, offsets, eighths)


def solution(mesh):
    sizes = tuple(mesh.shape[a] for a in ("gx", "gy", "gz"))
    block = P("gx", "gy", "gz")
    stacked = P(None, "gx", "gy", "gz")
    return jax.shard_map(
        functools.partial(step, sizes),
        mesh=mesh,
        in_specs=(stacked, block, stacked, stacked),
        out_specs=(stacked, block, block),
        check_vma=False,
    )
```

```python
import functools

import jax
import jax.numpy as jnp
from jax import lax
from jax.experimental import pallas as pl
from jax.experimental.pallas import tpu as pltpu
from jax.sharding import PartitionSpec as P

MESH = pl.DeviceIdType.MESH
RELAX = (6.0 / 7.0) / 6.0
HALO = 4
XY = [(dx, dy) for dx in (-1, 0, 1) for dy in (-1, 0, 1) if (dx, dy) != (0, 0)]


def lanes(shape):
    return lax.broadcasted_iota(jnp.int32, shape, len(shape) - 1)


def roll(x, shift, axis):
    shift = shift % x.shape[axis]
    return x if shift == 0 else pltpu.roll(x, shift, axis)


def inside(sizes, me, delta):
    ok = None
    for n, i, d in zip(sizes, me, delta):
        if d:
            one = (i + d >= 0) & (i + d < n)
            ok = one if ok is None else ok & one
    return ok


class Comm:
    def __init__(self, sizes, me, send, recv):
        self.sizes, self.me, self.send, self.recv = sizes, me, send, recv
        self.copies = []

    def add(self, delta, src, dst, slot):
        device = tuple(i + d for i, d in zip(self.me, delta))
        copy = pltpu.make_async_remote_copy(
            src_ref=src, dst_ref=dst, send_sem=self.send.at[slot], recv_sem=self.recv.at[slot],
            device_id=device, device_id_type=MESH,
        )
        to = inside(self.sizes, self.me, delta)
        source = inside(self.sizes, self.me, tuple(-d for d in delta))
        pl.when(to)(copy.start)
        self.copies.append((copy, to, source))

    def wait(self):
        for copy, to, source in self.copies:
            pl.when(source)(copy.wait_recv)
        for copy, to, source in self.copies:
            pl.when(to)(copy.wait_send)


def zero_if_missing(sizes, me, delta, ref):
    @pl.when(jnp.logical_not(inside(sizes, me, delta)))
    def _():
        ref[...] = jnp.zeros(ref.shape, ref.dtype)


def pick_x(d):
    return {-1: 0, 1: 1}[d]


def exchange_xy(sizes, me, own, strips, rx, ry, rc, sems, out, meanwhile=None):
    f, p, r, _ = own.shape
    hx, hy = rx.shape[2], ry.shape[3]
    for i in range(p):
        strips[0, :, i] = own[:, i, 0:hy, :]
        strips[1, :, i] = own[:, i, r - hy : r, :]
    comm = Comm(sizes, me, *sems)
    for slot, (dx, dy) in enumerate(XY):
        xs = slice(0, hx) if dx < 0 else slice(p - hx, p)
        if dy == 0:
            src, dst = own.at[:, xs], rx.at[pick_x(-dx)]
        elif dx == 0:
            src, dst = strips.at[pick_x(dy)], ry.at[pick_x(-dy)]
        else:
            src, dst = strips.at[pick_x(dy), :, xs], rc.at[pick_x(-dx), pick_x(-dy)]
        comm.add((dx, dy, 0), src, dst, slot)
    for dx, dy in XY:
        ref = rx.at[pick_x(dx)] if dy == 0 else ry.at[pick_x(dy)] if dx == 0 else rc.at[pick_x(dx), pick_x(dy)]
        zero_if_missing(sizes, me, (dx, dy, 0), ref)
    out[:, HALO : HALO + p, HALO : HALO + r, :] = own[...]
    if meanwhile is not None:
        meanwhile()
    comm.wait()
    for sx, xs in ((0, slice(HALO - hx, HALO)), (1, slice(HALO + p, HALO + p + hx))):
        out[:, xs, HALO : HALO + r, :] = rx[sx]
        for sy, ys in ((0, slice(HALO - hy, HALO)), (1, slice(HALO + r, HALO + r + hy))):
            out[:, xs, ys, :] = rc[sx, sy]
    for sy, ys in ((0, slice(HALO - hy, HALO)), (1, slice(HALO + r, HALO + r + hy))):
        out[:, HALO : HALO + p, ys, :] = ry[sy]


class ZExchange:
    def __init__(self, sizes, me, own, got, sems):
        self.comm = Comm(sizes, me, *sems)
        self.comm.add((0, 0, -1), own, got.at[1], 0)
        self.comm.add((0, 0, 1), own, got.at[0], 1)
        zero_if_missing(sizes, me, (0, 0, -1), got.at[0])
        zero_if_missing(sizes, me, (0, 0, 1), got.at[1])
        self.wait = self.comm.wait


def swap_blocks(regs, width, shift=0):
    n = len(regs)
    lane = lanes(regs[0].shape)
    into, outof = ((lane + shift) & 127) // width, lane // width
    bits = [1 << k for k in range(n.bit_length() - 1)]
    for bit in bits:
        mask = (into & bit) != 0
        regs = [jnp.where(mask, regs[(i + bit) % n], regs[i]) for i in range(n)]
    regs = [roll(regs[i], width * i + shift, 1) for i in range(n)]
    regs = [regs[-i % n] for i in range(n)]
    for bit in bits:
        mask = (outof & bit) != 0
        regs = [jnp.where(mask, regs[(i - bit) % n], regs[i]) for i in range(n)]
    return regs


def pack_z(ext, packed):
    f, p, rows, _ = ext.shape
    lane = lanes((rows, 128))
    for c in range(f):
        total = roll(ext[c, 0], 4, 1)
        for x in range(1, p):
            total = jnp.where(lane >= 8 * x, roll(ext[c, x], 4 + 8 * x, 1), total)
        packed[c] = total


def gather(x, index):
    return jnp.take_along_axis(x, index, axis=1, mode="promise_in_bounds")


def advect_block(v, load):
    lane = lanes((8, 128))
    part = (lane >> 3) & 1
    ox, oy, oz = v & 7, (v >> 3) & 7, (v >> 6) & 7
    fx = ((v >> 9) & 7).astype(jnp.float32) * 0.125
    fy = ((v >> 12) & 7).astype(jnp.float32) * 0.125
    fz = ((v >> 15) & 7).astype(jnp.float32) * 0.125
    spot = (lane & 7) + oz + part
    near = spot < 8
    first = ((lane >> 4) + ox) * 8 + (spot & 7)
    wz = jnp.where(part == 0, 1.0 - fz, fz)
    wy = [jnp.where(oy == dy, 1.0 - fy, jnp.where(oy == dy - 1, fy, 0.0)) for dy in range(9)]
    totals = []
    for cx in range(2):
        index = first + 8 * cx
        wx = (fx if cx else 1.0 - fx) * wz
        for c in range(4):
            total = None
            for dy in range(9):
                value = wy[dy] * jnp.where(near, gather(load(c, 0, dy), index), gather(load(c, 1, dy), index))
                total = value if total is None else total + value
            totals.append(wx * total)
    return [totals[c] + totals[4 + c] for c in range(4)]


def kernel(sizes, vel_hbm, den_hbm, off_hbm, eig_hbm, new_vel, new_den, press, off, eig, fetch_sem, fields, stripA, rxA, ryA, rcA, ext,
           edge, gotP, src, code, codeT, resT, u, stripB, rxB, ryB, rcB, extU, packU, gotU, wide, s0, q0, r0,
           tmp0, own1, strip1, rx1, ry1, rc1, ext1, got1, wide1, q1, r1, tmp1, own2, got2, ext2, gotz2, sum1, fine,
           sxyA, rxyA, szA, rzA, sxyB, rxyB, szB, rzB, sxy1, rxy1, sz1, rz1, sxy2, rxy2, sz2, rz2):
    me = tuple(lax.axis_index(a) for a in ("gx", "gy", "gz"))
    p, r = fields.shape[1], fields.shape[2]
    pairs = [(vel_hbm, fields.at[0:3]), (den_hbm, fields.at[3]), (off_hbm, off), (eig_hbm, eig)]
    fetch = [pltpu.make_async_copy(a, b, fetch_sem.at[i]) for i, (a, b) in enumerate(pairs)]
    for copy in fetch:
        copy.start()

    barrier = pltpu.get_barrier_semaphore()
    peers = [(dx, dy, 0) for dx, dy in XY] + [(0, 0, -1), (0, 0, 1)]
    count = jnp.int32(0)
    for delta in peers:
        ok = inside(sizes, me, delta)

        @pl.when(ok)
        def _():
            pl.semaphore_signal(barrier, inc=1, device_id=tuple(i + d for i, d in zip(me, delta)), device_id_type=MESH)

        count = count + jnp.where(ok, 1, 0)
    for copy in fetch[:2]:
        copy.wait()
    pl.semaphore_wait(barrier, count)

    even = ((lanes((8, 128)) >> 3) & 1) == 0

    def positions():
        for copy in fetch[2:]:
            copy.wait()
        whole = (off[0] + 4) + 8 * (off[1] + 4) + 64 * (off[2] + 4)
        code[...] = whole + 512 * eig[0] + 4096 * eig[1] + 32768 * eig[2]
        for t in range(r // 8):
            for q, v in enumerate(swap_blocks([code[x, 8 * t : 8 * t + 8] for x in range(p)], 16)):
                codeT[t, 2 * q] = jnp.where(even, v, roll(v, 8, 1))
                codeT[t, 2 * q + 1] = jnp.where(even, roll(v, -8, 1), v)

    exchange_xy(sizes, me, fields, stripA, rxA, ryA, rcA, (sxyA, rxyA), ext, positions)

    rows = r + 8
    tiles = rows // 8
    blocks = 128 // 8
    lane16 = lanes((r, 128))
    lane = lanes((rows, 128))

    def turn(c, carry):
        for t in range(tiles):
            for b, v in enumerate(swap_blocks([ext[c, x, 8 * t : 8 * t + 8] for x in range(p + 8)], 8, 4)):
                if b == 0:
                    edge[c, 8 * t : 8 * t + 8] = v
                else:
                    src[c, b, 8 * t : 8 * t + 8] = v
        return carry

    lax.fori_loop(0, 4, turn, 0)
    zA = ZExchange(sizes, me, edge, gotP, (szA, rzA))

    def advect(t, b):
        totals = advect_block(codeT[t, b], lambda c, far, dy: src[c, b + far, 8 * t + dy : 8 * t + dy + 8, :])
        for c in range(4):
            resT[c, t, b] = totals[c]

    def middle(i, carry):
        for half in range(2):
            for t in range(r // 8):
                advect(t, 2 * i + 1 + half)
        return carry

    lax.fori_loop(0, blocks // 2 - 1, middle, 0)
    zA.wait()
    low = (lane & 7) < 4
    for c in range(4):
        src[c, 0] = jnp.where(low, gotP[0, c], edge[c])
        src[c, blocks] = jnp.where(low, edge[c], gotP[1, c])
    for b in (0, blocks - 1):
        for t in range(r // 8):
            advect(t, b)

    def back(c, carry):
        for t in range(r // 8):
            pairs = []
            for q in range(blocks // 2):
                one, two = resT[c, t, 2 * q], resT[c, t, 2 * q + 1]
                move = jnp.where(even, two, one)
                pairs.append(jnp.where(even, one, two) + jnp.where(even, roll(move, -8, 1), roll(move, 8, 1)))
            for x, v in enumerate(swap_blocks(pairs, 16)):
                u[c, x, 8 * t : 8 * t + 8] = v
        return carry

    lax.fori_loop(0, 4, back, 0)
    new_den[...] = u[3]

    vel_u = u.at[0:3]
    exchange_xy(sizes, me, vel_u, stripB, rxB, ryB, rcB, (sxyB, rxyB), extU)
    pack_z(extU, packU)
    ZExchange(sizes, me, packU, gotU, (szB, rzB)).wait()
    for c in range(3):
        both = jnp.where((lane & 7) < 4, gotU[0, c], gotU[1, c])
        for x in range(HALO - 3, HALO + p + 3):
            wide[c, x, :, 0:128] = extU[c, x]
            wide[c, x, :, 128:256] = roll(both, -(8 * x + 4), 1)

    def yz_mask(nrows, first_row, block_rows, cells):
        row = lax.broadcasted_iota(jnp.int32, (nrows, 256), 0) - first_row + me[1] * block_rows
        spot = lanes((nrows, 256))
        z = jnp.where(spot < 192, spot, spot - 256) + me[2] * cells
        return (row >= 0) & (row < sizes[1] * block_rows) & (z >= 0) & (z < sizes[2] * cells)

    def x_ok(x, first, block):
        g = x - first + me[0] * block
        return (g >= 0) & (g < sizes[0] * block)

    mask0 = yz_mask(rows, HALO, r, 128)

    def around(ref, x, step):
        v = ref[x]
        total = ref[x + 1] + ref[x - 1]
        total = total + roll(v, -1, 0) + roll(v, 1, 0)
        total = total + roll(v, -step, 1) + roll(v, step, 1)
        return 6.0 * v - total

    def second(ref, x, scale, step):
        v = ref[x]
        first = (RELAX * scale) * v
        return first + RELAX * (scale * v - (RELAX * scale) * around(ref, x, step))

    def source0(x, carry):
        part = wide[0, x + 1] - wide[0, x - 1]
        v = wide[1, x]
        part = part + (roll(v, -1, 0) - roll(v, 1, 0))
        v = wide[2, x]
        part = part + (roll(v, -1, 1) - roll(v, 1, 1))
        s0[x] = jnp.where(mask0 & x_ok(x, HALO, p), -0.5 * part, 0.0)
        return carry

    lax.fori_loop(HALO - 2, HALO + p + 2, source0, 0)

    def second0(x, carry):
        q0[x] = jnp.where(mask0 & x_ok(x, HALO, p), second(s0, x, 1.0, 1), 0.0)
        return carry

    lax.fori_loop(HALO - 1, HALO + p + 1, second0, 0)

    def residual0(x, carry):
        r0[x] = (s0[x] - around(q0, x, 1))[:, 0:128]
        return carry

    lax.fori_loop(HALO, HALO + p, residual0, 0)
    lane8 = lanes((r // 2, 128))
    for x in range(p // 2):
        tmp0[...] = r0[HALO + 2 * x] + r0[HALO + 2 * x + 1]
        v = tmp0[pl.ds(HALO, r // 2, stride=2), :] + tmp0[pl.ds(HALO + 1, r // 2, stride=2), :]
        v = v + jnp.where((lane8 & 1) == 0, roll(v, -1, 1), roll(v, 1, 1))
        own1[0, x] = 0.125 * v

    p1, r1n = p // 2, r // 2
    exchange_xy(sizes, me, own1, strip1, rx1, ry1, rc1, (sxy1, rxy1), ext1)
    near1 = pl.ds(HALO - 2, p1 + 4)
    ZExchange(sizes, me, ext1.at[0, near1], got1, (sz1, rz1)).wait()
    rows1 = r1n + 8
    lane1 = lanes((rows1, 128))
    for x in range(HALO - 2, HALO + p1 + 2):
        wide1[x, :, 0:128] = ext1[0, x]
        wide1[x, :, 128:256] = jnp.where(lane1 < 64, got1[1, x - HALO + 2], got1[0, x - HALO + 2])
    mask1 = yz_mask(rows1, HALO, r1n, 128)
    for x in range(HALO - 1, HALO + p1 + 1):
        q1[x] = jnp.where(mask1 & x_ok(x, HALO, p1), second(wide1, x, 4.0, 2), 0.0)
    for x in range(HALO, HALO + p1):
        r1[x] = (wide1[x] - 0.25 * around(q1, x, 2))[:, 0:128]
    p2, r2n = p1 // 2, r1n // 2
    lane4 = lanes((r2n, 128))
    for x in range(p2):
        tmp1[...] = r1[HALO + 2 * x] + r1[HALO + 2 * x + 1]
        v = tmp1[pl.ds(HALO, r2n, stride=2), :] + tmp1[pl.ds(HALO + 1, r2n, stride=2), :]
        v = v + jnp.where((lane4 & 3) < 2, roll(v, -2, 1), roll(v, 2, 1))
        own2[x] = 0.125 * v

    comm = Comm(sizes, me, sxy2, rxy2)
    for slot, (dx, dy) in enumerate(XY):
        comm.add((dx, dy, 0), own2, got2.at[1 - dx, 1 - dy], slot)
    for dx, dy in XY:
        zero_if_missing(sizes, me, (dx, dy, 0), got2.at[dx + 1, dy + 1])
    got2[1, 1] = own2[...]
    ext2[...] = jnp.zeros(ext2.shape, jnp.float32)
    comm.wait()
    for a in range(3):
        for b in range(3):
            ext2[p2 * a : p2 * a + p2, r2n * b : r2n * b + r2n, :] = got2[a, b]
    ZExchange(sizes, me, ext2, gotz2, (sz2, rz2)).wait()
    lane2 = lanes((16, 128))
    mask2 = yz_mask(16, r2n, r2n, 128)
    planes2 = {}
    for x in range(p2 - 2, 2 * p2 + 2):
        planes2[x] = jnp.concatenate([ext2[x], jnp.where(lane2 < 64, gotz2[1, x], gotz2[0, x])], axis=1)
    sum1[...] = jnp.zeros(sum1.shape, jnp.float32)
    for x in range(p2 - 1, 2 * p2 + 1):
        v = jnp.where(mask2 & x_ok(x, p2, p2), second(planes2, x, 16.0, 4), 0.0)
        first_row = r2n - 1
        take = r2n + 2
        base = HALO - 2
        for side in range(2):
            part = v[first_row : first_row + take, 128 * side : 128 * side + 128]
            sum1[x, side, pl.ds(base, take, stride=2), :] = part
            sum1[x, side, pl.ds(base + 1, take, stride=2), :] = part
    for x1 in range(HALO - 1, HALO + p1 + 1):
        x2 = (x1 - HALO) // 2 + p2
        for side in range(2):
            v = q1[x1, :, 128 * side : 128 * side + 128] + sum1[x2, side]
            part = v[HALO - 2 : HALO - 2 + r1n + 4]
            fine[x1, side, pl.ds(0, r1n + 4, stride=2), :] = part
            fine[x1, side, pl.ds(1, r1n + 4, stride=2), :] = part
    for x in range(HALO - 1, HALO + p + 1):
        x1 = (x - HALO) // 2 + HALO
        coarse = jnp.concatenate([fine[x1, 0], fine[x1, 1]], axis=1)
        s0[x] = jnp.where(mask0 & x_ok(x, HALO, p), q0[x] + coarse, 0.0)
    for x in range(p):
        v = s0[x + HALO]
        cut = lambda t: t[HALO : HALO + r, 0:128]
        press[x] = cut(v)
        new_vel[0, x] = u[0, x] - 0.5 * cut(s0[x + HALO + 1] - s0[x + HALO - 1])
        new_vel[1, x] = u[1, x] - 0.5 * cut(roll(v, -1, 0) - roll(v, 1, 0))
        new_vel[2, x] = u[2, x] - 0.5 * cut(roll(v, -1, 1) - roll(v, 1, 1))


def step(sizes, velocity, density, offsets, eighths):
    p, r, _ = density.shape
    f32 = jnp.float32

    def vm(*shape):
        return pltpu.VMEM(shape, f32)

    def xy(f, p, r, hx, hy):
        return [vm(2, f, p, hy, 128), vm(2, f, hx, r, 128), vm(2, f, p, hy, 128), vm(2, 2, f, hx, hy, 128)]

    assert p == 8 and r % 8 == 0
    p1, r1, p2, r2 = p // 2, r // 2, p // 4, r // 4
    rows, rows1 = r + 8, r1 + 8
    dma = lambda n: pltpu.SemaphoreType.DMA((n,))
    scratch = (
        [pltpu.VMEM(offsets.shape, jnp.int32), pltpu.VMEM(eighths.shape, jnp.int32), dma(4), vm(4, p, r, 128)] + xy(4, p, r, 4, 4)
        + [vm(4, p + 8, rows, 128), vm(4, rows, 128), vm(2, 4, rows, 128), vm(4, 17, rows, 128),
           pltpu.VMEM((p, r, 128), jnp.int32), pltpu.VMEM((r // 8, 16, 8, 128), jnp.int32),
           vm(4, r // 8, 16, 8, 128), vm(4, p, r, 128)]
        + xy(3, p, r, 3, 4)
        + [vm(3, p + 8, rows, 128), vm(3, rows, 128), vm(2, 3, rows, 128), vm(3, p + 8, rows, 256),
           vm(p + 8, rows, 256), vm(p + 8, rows, 256), vm(p + 8, rows, 128), vm(rows, 128), vm(1, p1, r1, 128)]
        + xy(1, p1, r1, 2, 2)
        + [vm(1, p1 + 8, rows1, 128), vm(2, p1 + 4, rows1, 128), vm(p1 + 8, rows1, 256), vm(p1 + 8, rows1, 256),
           vm(p1 + 8, rows1, 128), vm(rows1, 128), vm(p2, r2, 128), vm(3, 3, p2, r2, 128), vm(3 * p2, 16, 128),
           vm(2, 3 * p2, 16, 128), vm(3 * p2, 2, rows1, 128), vm(p1 + 8, 2, rows, 128)]
        + [dma(8), dma(8), dma(2), dma(2)] * 4
    )
    vmem = pl.BlockSpec(memory_space=pltpu.VMEM)
    return pl.pallas_call(
        functools.partial(kernel, sizes),
        out_shape=(
            jax.ShapeDtypeStruct(velocity.shape, f32),
            jax.ShapeDtypeStruct(density.shape, f32),
            jax.ShapeDtypeStruct(density.shape, f32),
        ),
        in_specs=[pl.BlockSpec(memory_space=pltpu.HBM)] * 4,
        out_specs=(vmem,) * 3,
        scratch_shapes=scratch,
        compiler_params=pltpu.CompilerParams(
            collective_id=0, has_side_effects=True, vmem_limit_bytes=60 * 1024 * 1024
        ),
    )(velocity, density, offsets, eighths)


def solution(mesh):
    sizes = tuple(mesh.shape[a] for a in ("gx", "gy", "gz"))
    block = P("gx", "gy", "gz")
    stacked = P(None, "gx", "gy", "gz")
    return jax.shard_map(
        functools.partial(step, sizes),
        mesh=mesh,
        in_specs=(stacked, block, stacked, stacked),
        out_specs=(stacked, block, block),
        check_vma=False,
    )
```

```python
import functools

import jax
import jax.numpy as jnp
from jax import lax
from jax.experimental import pallas as pl
from jax.experimental.pallas import tpu as pltpu
from jax.sharding import PartitionSpec as P

MESH = pl.DeviceIdType.MESH
RELAX = (6.0 / 7.0) / 6.0
HALO = 4
XY = [(-1, -1), (-1, 1), (1, -1), (1, 1), (-1, 0), (1, 0), (0, -1), (0, 1)]


def lanes(shape):
    return lax.broadcasted_iota(jnp.int32, shape, len(shape) - 1)


def roll(x, shift, axis):
    shift = shift % x.shape[axis]
    return x if shift == 0 else pltpu.roll(x, shift, axis)


def inside(sizes, me, delta):
    ok = None
    for n, i, d in zip(sizes, me, delta):
        if d:
            one = (i + d >= 0) & (i + d < n)
            ok = one if ok is None else ok & one
    return ok


class Comm:
    def __init__(self, sizes, me, send, recv):
        self.sizes, self.me, self.send, self.recv_sem = sizes, me, send, recv
        self.copies = []

    def add(self, delta, src, dst):
        slot = len(self.copies)
        device = tuple(i + d for i, d in zip(self.me, delta))
        copy = pltpu.make_async_remote_copy(
            src_ref=src, dst_ref=dst, send_sem=self.send.at[slot], recv_sem=self.recv_sem.at[slot],
            device_id=device, device_id_type=MESH,
        )
        to = inside(self.sizes, self.me, delta)
        source = inside(self.sizes, self.me, tuple(-d for d in delta))
        self.copies.append((copy, to, source, dst))

    def missing(self):
        for copy, to, source, dst in self.copies:

            @pl.when(jnp.logical_not(source))
            def _(dst=dst):
                dst[...] = jnp.zeros(dst.shape, dst.dtype)

    def start(self):
        for copy, to, source, dst in self.copies:
            pl.when(to)(copy.start)

    def recv(self, first=0, last=None):
        for copy, to, source, dst in self.copies[first:last]:
            pl.when(source)(copy.wait_recv)

    def sent(self):
        for copy, to, source, dst in self.copies:
            pl.when(to)(copy.wait_send)


def pick(d):
    return {-1: 0, 1: 1}[d]


def cut_strips(own, strips):
    f, p, r, _ = own.shape
    hy = strips.shape[3]
    for i in range(p):
        strips[0, :, i] = own[:, i, 0:hy, :]
        strips[1, :, i] = own[:, i, r - hy : r, :]


def add_xy(comm, own, strips, bufs, dz=0):
    rx, ry, rc = bufs
    p, hx = own.shape[1], rx.shape[2]
    for dx, dy in XY:
        xs = slice(0, hx) if dx < 0 else slice(p - hx, p)
        if dy == 0:
            src, dst = own.at[:, xs], rx.at[pick(-dx)]
        elif dx == 0:
            src, dst = strips.at[pick(dy)], ry.at[pick(-dy)]
        else:
            src, dst = strips.at[pick(dy), :, xs], rc.at[pick(-dx), pick(-dy)]
        comm.add((dx, dy, dz), src, dst)


def frame_halo(bufs, p, r, out):
    rx, ry, rc = bufs
    hx, hy = rx.shape[2], ry.shape[3]
    for sx, xs in ((0, slice(HALO - hx, HALO)), (1, slice(HALO + p, HALO + p + hx))):
        out[:, xs, HALO : HALO + r, :] = rx[sx]
        for sy, ys in ((0, slice(HALO - hy, HALO)), (1, slice(HALO + r, HALO + r + hy))):
            out[:, xs, ys, :] = rc[sx, sy]
    for sy, ys in ((0, slice(HALO - hy, HALO)), (1, slice(HALO + r, HALO + r + hy))):
        out[:, HALO : HALO + p, ys, :] = ry[sy]


def swap_blocks(regs, width, shift=0):
    n = len(regs)
    lane = lanes(regs[0].shape)
    into, outof = ((lane + shift) & 127) // width, lane // width
    bits = [1 << k for k in range(n.bit_length() - 1)]
    for bit in bits:
        mask = (into & bit) != 0
        regs = [jnp.where(mask, regs[(i + bit) % n], regs[i]) for i in range(n)]
    regs = [roll(regs[i], width * i + shift, 1) for i in range(n)]
    regs = [regs[-i % n] for i in range(n)]
    for bit in bits:
        mask = (outof & bit) != 0
        regs = [jnp.where(mask, regs[(i - bit) % n], regs[i]) for i in range(n)]
    return regs


def gather(x, index):
    return jnp.take_along_axis(x, index, axis=1, mode="promise_in_bounds")


def plan_block(v, place, weight):
    lane = lanes((8, 128))
    part = (lane >> 3) & 1
    ox, oy, oz = v & 7, (v >> 3) & 7, (v >> 6) & 7
    fx = ((v >> 9) & 7).astype(jnp.float32) * 0.125
    fy = ((v >> 12) & 7).astype(jnp.float32) * 0.125
    fz = ((v >> 15) & 7).astype(jnp.float32) * 0.125
    spot = (lane & 7) + oz + part
    place[0] = ((lane >> 4) + ox) * 8 + (spot & 7)
    place[1] = spot
    wz = jnp.where(part == 0, 1.0 - fz, fz)
    for dy in range(9):
        weight[dy] = jnp.where(oy == dy, 1.0 - fy, jnp.where(oy == dy - 1, fy, 0.0))
    weight[9] = (1.0 - fx) * wz
    weight[10] = fx * wz


def advect_block(place, weight, steps, load):
    near = place[1] < 8
    result = None
    for cx in range(2):
        index = place[0] + 8 * cx
        total = None
        for dy in steps:
            value = weight[dy] * jnp.where(near, gather(load(0, dy), index), gather(load(1, dy), index))
            total = value if total is None else total + value
        total = weight[9 + cx] * total
        result = total if result is None else result + total
    return result


def kernel(sizes, vel_hbm, den_hbm, off_hbm, eig_hbm, new_vel, new_den, press, off, eig, fetch_sem, fields, stripA, rxA, ryA, rcA, mixed,
           edge, gotP, src, code, place, weight, resT, u, extU, packU, wide, s0, q0, r0,
           tmp0, own1, strip1, rx1, ry1, rc1, rz1, ext1, wide1, q1, r1, tmp1, own2, got2, ext2, sum1, fine,
           sA, rA, szA, rzA, sB, rB, sC, rC, sD, rD, *bufB):
    me = tuple(lax.axis_index(a) for a in ("gx", "gy", "gz"))
    p, r = fields.shape[1], fields.shape[2]
    p1, r1n = p // 2, r // 2
    p2, r2n = p1 // 2, r1n // 2
    pairs = [(vel_hbm, fields.at[0:3]), (den_hbm, fields.at[3]), (off_hbm, off), (eig_hbm, eig)]
    fetch = [pltpu.make_async_copy(a, b, fetch_sem.at[i]) for i, (a, b) in enumerate(pairs)]
    for copy in fetch:
        copy.start()

    barrier = pltpu.get_barrier_semaphore()
    peers = [(dx, dy, dz) for dz in (-1, 0, 1) for dx in (-1, 0, 1) for dy in (-1, 0, 1) if (dx, dy, dz) != (0, 0, 0)]
    count = jnp.int32(0)
    for delta in peers:
        ok = inside(sizes, me, delta)

        @pl.when(ok)
        def _():
            pl.semaphore_signal(barrier, inc=1, device_id=tuple(i + d for i, d in zip(me, delta)), device_id_type=MESH)

        count = count + jnp.where(ok, 1, 0)

    sendA = [Comm(sizes, me, sA.at[i], rA.at[i]) for i in range(3)]
    for c in range(4):
        for dx in (-1, 1):
            xs = slice(0, HALO) if dx < 0 else slice(p - HALO, p)
            sendA[0].add((dx, 0, 0), fields.at[c, xs], rxA.at[pick(-dx), c])
            sendA[1].add((0, dx, 0), stripA.at[pick(dx), c], ryA.at[pick(-dx), c])
            for dy in (-1, 1):
                sendA[2].add((dx, dy, 0), stripA.at[pick(dy), c, xs], rcA.at[pick(-dx), pick(-dy), c])
    zA = Comm(sizes, me, szA, rzA)
    for c in range(4):
        zA.add((0, 0, -1), edge.at[c], gotP.at[1, c])
        zA.add((0, 0, 1), edge.at[c], gotP.at[0, c])
    fieldB = [bufB[8 * c : 8 * c + 8] for c in range(3)]
    commB = [Comm(sizes, me, sB.at[c], rB.at[c]) for c in range(3)]
    for c, (strip, rx, ry, rc, edgeB, estrB, ezB, ezyB) in enumerate(fieldB):
        add_xy(commB[c], u.at[c : c + 1], strip, (rx, ry, rc))
        for dz in (-1, 1):
            for dx in (-1, 1, 0):
                for dy in (-1, 1):
                    commB[c].add((dx, dy, dz), estrB.at[pick(dy)], ezyB.at[pick(-dz), 1 - dx, pick(-dy)])
                commB[c].add((dx, 0, dz), edgeB, ezB.at[pick(-dz), 1 - dx])
    commC = Comm(sizes, me, sC, rC)
    commD = Comm(sizes, me, sD, rD)
    for dz in (-1, 1, 0):
        add_xy(commC, own1, strip1, (rx1.at[1 - dz], ry1.at[1 - dz], rc1.at[1 - dz]), dz)
        for dx, dy in XY:
            commD.add((dx, dy, dz), own2, got2.at[1 - dz, 1 - dx, 1 - dy])
        if dz:
            commC.add((0, 0, dz), own1, rz1.at[pick(-dz)])
            commD.add((0, 0, dz), own2, got2.at[1 - dz, 1, 1])
    comms = sendA + [zA] + commB + [commC, commD]
    for comm in comms:
        comm.missing()
    ext2[...] = jnp.zeros(ext2.shape, jnp.float32)
    sum1[...] = jnp.zeros(sum1.shape, jnp.float32)
    for copy in fetch[:2]:
        copy.wait()
    cut_strips(fields, stripA)
    pl.semaphore_wait(barrier, count)
    for comm in sendA:
        comm.start()

    even = ((lanes((8, 128)) >> 3) & 1) == 0

    def positions():
        for copy in fetch[2:]:
            copy.wait()
        whole = (off[0] + 4) + 8 * (off[1] + 4) + 64 * (off[2] + 4)
        code[...] = whole + 512 * eig[0] + 4096 * eig[1] + 32768 * eig[2]
        for t in range(r // 8):
            for q, v in enumerate(swap_blocks([code[x, 8 * t : 8 * t + 8] for x in range(p)], 16)):
                code[q, 8 * t : 8 * t + 8] = v
        for t in range(r // 8):

            def plan(q, carry):
                v = code[q, 8 * t : 8 * t + 8]
                plan_block(jnp.where(even, v, roll(v, 8, 1)), place.at[t, 2 * q], weight.at[t, 2 * q])
                plan_block(jnp.where(even, roll(v, -8, 1), v), place.at[t, 2 * q + 1], weight.at[t, 2 * q + 1])
                return carry

            lax.fori_loop(0, 8, plan, 0)

    positions()
    rows = r + 8
    blocks = 128 // 8
    half = r // 8
    lane16 = lanes((r, 128))
    lane = lanes((rows, 128))
    near_steps = [[dy for dy in range(9) if 0 <= 8 * t + dy - 4 <= r - 8] for t in range(half)]
    far_steps = [[dy for dy in range(9) if dy not in near_steps[t]] for t in range(half)]

    def advect(c, t, b, steps):
        return advect_block(place.at[t, b], weight.at[t, b], steps, lambda far, dy: src[c, b + far, 8 * t + 4 + dy : 8 * t + 12 + dy, :])

    def put(c, b, start, size, v):
        if b == 0:
            edge[c, start : start + size] = v
        else:
            src[c, b, start : start + size] = v

    def first(c, carry):
        for dx in (-1, 1):
            xs = slice(0, HALO) if dx < 0 else slice(p - HALO, p)
            copy = pltpu.make_async_remote_copy(
                src_ref=fields.at[c, xs], dst_ref=rxA.at[pick(-dx), c], send_sem=sA.at[0, 2 * c + pick(dx)],
                recv_sem=rA.at[0, 2 * c + pick(dx)], device_id=tuple(i + d for i, d in zip(me, (dx, 0, 0))), device_id_type=MESH,
            )
            pl.when(inside(sizes, me, (-dx, 0, 0)))(copy.wait_recv)
        for t in range(half):
            ys = slice(8 * t, 8 * t + 8)
            planes = [rxA[0, c, x, ys] for x in range(HALO)] + [fields[c, x, ys] for x in range(p)] + [rxA[1, c, x, ys] for x in range(HALO)]
            for b, v in enumerate(swap_blocks(planes, 8, 4)):
                put(c, b, 8 + 8 * t, 8, v)
        for b in range(1, blocks - 1):
            for t in range(half):
                resT[c, t, b] = advect(c, t, b, near_steps[t])
        return carry

    lax.fori_loop(0, 4, first, 0)
    sendA[1].recv()
    sendA[2].recv()

    def turn(c, carry):
        for side, at in ((1, 0), (0, 4)):
            for x in range(HALO):
                mixed[c, x, at : at + 4] = rcA[0, side, c, x]
                mixed[c, HALO + p + x, at : at + 4] = rcA[1, side, c, x]
            for x in range(p):
                mixed[c, HALO + x, at : at + 4] = ryA[side, c, x]
        for b, v in enumerate(swap_blocks([mixed[c, x] for x in range(p + 8)], 8, 4)):
            put(c, b, 4, 4, v[4:8])
            put(c, b, r + 8, 4, v[0:4])
        return carry

    lax.fori_loop(0, 4, turn, 0)
    zA.start()
    low = (lanes((r + 16, 128)) & 7) < 4
    for c in range(4):
        for b in range(1, blocks - 1):
            for t in range(half):
                resT[c, t, b] = resT[c, t, b] + advect(c, t, b, far_steps[t])
        zA.recv(2 * c, 2 * c + 2)
        src[c, 0] = jnp.where(low, gotP[0, c], edge[c])
        src[c, blocks] = jnp.where(low, edge[c], gotP[1, c])
        for b in (0, blocks - 1):
            for t in range(half):
                resT[c, t, b] = advect(c, t, b, range(9))
        for t in range(half):
            pairs = []
            for q in range(blocks // 2):
                one, two = resT[c, t, 2 * q], resT[c, t, 2 * q + 1]
                move = jnp.where(even, two, one)
                pairs.append(jnp.where(even, one, two) + jnp.where(even, roll(move, -8, 1), roll(move, 8, 1)))
            for x, v in enumerate(swap_blocks(pairs, 16)):
                u[c, x, 8 * t : 8 * t + 8] = v
        if c == 3:
            new_den[...] = u[3]
            break
        strip, rx, ry, rc, edgeB, estrB, ezB, ezyB = fieldB[c]
        cut_strips(u.at[c : c + 1], strip)
        total = roll(u[c, 0], 4, 1)
        for x in range(1, p):
            total = jnp.where(lane16 >= 8 * x, roll(u[c, x], 4 + 8 * x, 1), total)
        edgeB[...] = total
        estrB[0] = total[0 : estrB.shape[1]]
        estrB[1] = total[r - estrB.shape[1] : r]
        commB[c].start()

    extU[:, HALO : HALO + p, HALO : HALO + r, :] = u[0:3]
    for c in range(3):
        commB[c].recv()

    def edges(lo, hi):
        spot = lanes(lo[0].shape)
        v = [jnp.where((spot & 7) < 4, lo[i], hi[i]) for i in range(3)]
        return jnp.where(spot < 32, roll(v[0], -32, 1), jnp.where(spot < 96, roll(v[1], 32, 1), roll(v[2], 96, 1)))

    for c, (strip, rx, ry, rc, edgeB, estrB, ezB, ezyB) in enumerate(fieldB):
        frame_halo((rx, ry, rc), p, r, extU.at[c : c + 1])
        hy = estrB.shape[1]
        packU[c, HALO : HALO + r] = edges([ezB[0, i] for i in range(3)], [ezB[1, i] for i in range(3)])
        for sy, ys in ((0, slice(HALO - hy, HALO)), (1, slice(HALO + r, HALO + r + hy))):
            packU[c, ys] = edges([ezyB[0, i, sy] for i in range(3)], [ezyB[1, i, sy] for i in range(3)])
    for c in range(3):
        for x in range(HALO - 3, HALO + p + 3):
            wide[c, x, :, 0:128] = extU[c, x]
            wide[c, x, :, 128:256] = roll(packU[c], -(8 * x + 4), 1)

    def yz_mask(nrows, first_row, block_rows, cells):
        row = lax.broadcasted_iota(jnp.int32, (nrows, 256), 0) - first_row + me[1] * block_rows
        spot = lanes((nrows, 256))
        z = jnp.where(spot < 192, spot, spot - 256) + me[2] * cells
        return (row >= 0) & (row < sizes[1] * block_rows) & (z >= 0) & (z < sizes[2] * cells)

    def x_ok(x, first, block):
        g = x - first + me[0] * block
        return (g >= 0) & (g < sizes[0] * block)

    mask0 = yz_mask(rows, HALO, r, 128)

    def around(ref, x, step):
        v = ref[x]
        total = ref[x + 1] + ref[x - 1]
        total = total + roll(v, -1, 0) + roll(v, 1, 0)
        total = total + roll(v, -step, 1) + roll(v, step, 1)
        return 6.0 * v - total

    def second(ref, x, scale, step):
        v = ref[x]
        first = (RELAX * scale) * v
        return first + RELAX * (scale * v - (RELAX * scale) * around(ref, x, step))

    def source0(x, carry):
        part = wide[0, x + 1] - wide[0, x - 1]
        v = wide[1, x]
        part = part + (roll(v, -1, 0) - roll(v, 1, 0))
        v = wide[2, x]
        part = part + (roll(v, -1, 1) - roll(v, 1, 1))
        s0[x] = jnp.where(mask0 & x_ok(x, HALO, p), -0.5 * part, 0.0)
        return carry

    lax.fori_loop(HALO - 2, HALO + p + 2, source0, 0)

    def second0(x, carry):
        q0[x] = jnp.where(mask0 & x_ok(x, HALO, p), second(s0, x, 1.0, 1), 0.0)
        return carry

    lax.fori_loop(HALO - 1, HALO + p + 1, second0, 0)

    def residual0(x, carry):
        r0[x] = (s0[x] - around(q0, x, 1))[:, 0:128]
        return carry

    lax.fori_loop(HALO, HALO + p, residual0, 0)
    lane8 = lanes((r // 2, 128))
    for x in range(p // 2):
        tmp0[...] = r0[HALO + 2 * x] + r0[HALO + 2 * x + 1]
        v = tmp0[pl.ds(HALO, r // 2, stride=2), :] + tmp0[pl.ds(HALO + 1, r // 2, stride=2), :]
        v = v + jnp.where((lane8 & 1) == 0, roll(v, -1, 1), roll(v, 1, 1))
        own1[0, x] = 0.125 * v

    cut_strips(own1, strip1)
    commC.start()
    commC.recv()
    rows1 = r1n + 8
    for dz in range(3):
        ext1[dz, :, HALO : HALO + p1, HALO : HALO + r1n, :] = own1[...] if dz == 1 else rz1[dz // 2]
        frame_halo((rx1.at[dz], ry1.at[dz], rc1.at[dz]), p1, r1n, ext1.at[dz])
    lane1 = lanes((rows1, 128))
    for x in range(HALO - 2, HALO + p1 + 2):
        wide1[x, :, 0:128] = ext1[1, 0, x]
        wide1[x, :, 128:256] = jnp.where(lane1 < 64, ext1[2, 0, x], ext1[0, 0, x])
    mask1 = yz_mask(rows1, HALO, r1n, 128)
    for x in range(HALO - 1, HALO + p1 + 1):
        q1[x] = jnp.where(mask1 & x_ok(x, HALO, p1), second(wide1, x, 4.0, 2), 0.0)
    for x in range(HALO, HALO + p1):
        r1[x] = (wide1[x] - 0.25 * around(q1, x, 2))[:, 0:128]
    lane4 = lanes((r2n, 128))
    for x in range(p2):
        tmp1[...] = r1[HALO + 2 * x] + r1[HALO + 2 * x + 1]
        v = tmp1[pl.ds(HALO, r2n, stride=2), :] + tmp1[pl.ds(HALO + 1, r2n, stride=2), :]
        v = v + jnp.where((lane4 & 3) < 2, roll(v, -2, 1), roll(v, 2, 1))
        own2[x] = 0.125 * v

    commD.start()
    got2[1, 1, 1] = own2[...]
    commD.recv()
    for z in range(3):
        for a in range(3):
            for b in range(3):
                ext2[z, p2 * a : p2 * a + p2, r2n * b : r2n * b + r2n, :] = got2[z, a, b]
    lane2 = lanes((16, 128))
    mask2 = yz_mask(16, r2n, r2n, 128)
    planes2 = {}
    for x in range(p2 - 2, 2 * p2 + 2):
        planes2[x] = jnp.concatenate([ext2[1, x], jnp.where(lane2 < 64, ext2[2, x], ext2[0, x])], axis=1)
    for x in range(p2 - 1, 2 * p2 + 1):
        v = jnp.where(mask2 & x_ok(x, p2, p2), second(planes2, x, 16.0, 4), 0.0)
        first_row = r2n - 1
        take = r2n + 2
        base = HALO - 2
        for side in range(2):
            part = v[first_row : first_row + take, 128 * side : 128 * side + 128]
            sum1[x, side, pl.ds(base, take, stride=2), :] = part
            sum1[x, side, pl.ds(base + 1, take, stride=2), :] = part
    for x1 in range(HALO - 1, HALO + p1 + 1):
        x2 = (x1 - HALO) // 2 + p2
        for side in range(2):
            v = q1[x1, :, 128 * side : 128 * side + 128] + sum1[x2, side]
            part = v[HALO - 2 : HALO - 2 + r1n + 4]
            fine[x1, side, pl.ds(0, r1n + 4, stride=2), :] = part
            fine[x1, side, pl.ds(1, r1n + 4, stride=2), :] = part
    for x in range(HALO - 1, HALO + p + 1):
        x1 = (x - HALO) // 2 + HALO
        coarse = jnp.concatenate([fine[x1, 0], fine[x1, 1]], axis=1)
        s0[x] = jnp.where(mask0 & x_ok(x, HALO, p), q0[x] + coarse, 0.0)
    for x in range(p):
        v = s0[x + HALO]
        cut = lambda t: t[HALO : HALO + r, 0:128]
        press[x] = cut(v)
        new_vel[0, x] = u[0, x] - 0.5 * cut(s0[x + HALO + 1] - s0[x + HALO - 1])
        new_vel[1, x] = u[1, x] - 0.5 * cut(roll(v, -1, 0) - roll(v, 1, 0))
        new_vel[2, x] = u[2, x] - 0.5 * cut(roll(v, -1, 1) - roll(v, 1, 1))
    for comm in comms:
        comm.sent()


def write_kernel(*refs):
    n = len(refs) // 2
    copies = [pltpu.make_async_copy(refs[i], refs[n + i], refs[-1].at[i]) for i in range(n)]
    for copy in copies:
        copy.start()
    for copy in copies:
        copy.wait()


def write_out(results):
    return pl.pallas_call(
        write_kernel,
        out_shape=tuple(jax.ShapeDtypeStruct(a.shape, a.dtype) for a in results),
        in_specs=[pl.BlockSpec(memory_space=pltpu.VMEM)] * len(results),
        out_specs=(pl.BlockSpec(memory_space=pltpu.HBM),) * len(results),
        scratch_shapes=[pltpu.SemaphoreType.DMA((len(results),))],
        compiler_params=pltpu.CompilerParams(vmem_limit_bytes=1 << 20),
    )(*results)


def step(sizes, velocity, density, offsets, eighths):
    p, r, _ = density.shape
    f32 = jnp.float32

    def vm(*shape):
        return pltpu.VMEM(shape, f32)

    def xy(f, p, r, hx, hy):
        return [vm(2, f, p, hy, 128), vm(2, f, hx, r, 128), vm(2, f, p, hy, 128), vm(2, 2, f, hx, hy, 128)]

    assert p == 8 and r % 8 == 0
    p1, r1, p2, r2 = p // 2, r // 2, p // 4, r // 4
    rows, rows1 = r + 8, r1 + 8
    dma = lambda *n: pltpu.SemaphoreType.DMA(n)
    half = r // 8
    scratch = (
        [pltpu.VMEM(offsets.shape, jnp.int32), pltpu.VMEM(eighths.shape, jnp.int32), dma(4), vm(4, p, r, 128)] + xy(4, p, r, 4, 4)
        + [vm(4, p + 8, 8, 128), vm(4, r + 16, 128), vm(2, 4, r + 16, 128), vm(4, 17, r + 16, 128),
           pltpu.VMEM((p, r, 128), jnp.int32), pltpu.VMEM((half, 16, 2, 8, 128), jnp.int32), vm(half, 16, 11, 8, 128),
           vm(4, half, 16, 8, 128), vm(4, p, r, 128)]
        + [vm(3, p + 8, rows, 128), vm(3, rows, 128), vm(3, p + 8, rows, 256),
           vm(p + 8, rows, 256), vm(p + 8, rows, 256), vm(p + 8, rows, 128), vm(rows, 128), vm(1, p1, r1, 128)]
        + [vm(2, 1, p1, 2, 128), vm(3, 2, 1, 2, r1, 128), vm(3, 2, 1, p1, 2, 128), vm(3, 2, 2, 1, 2, 2, 128), vm(2, 1, p1, r1, 128)]
        + [vm(3, 1, p1 + 8, rows1, 128), vm(p1 + 8, rows1, 256), vm(p1 + 8, rows1, 256),
           vm(p1 + 8, rows1, 128), vm(rows1, 128), vm(p2, r2, 128), vm(3, 3, 3, p2, r2, 128), vm(3, 3 * p2, 16, 128),
           vm(3 * p2, 2, rows1, 128), vm(p1 + 8, 2, rows, 128)]
        + [dma(3, 16), dma(3, 16), dma(8), dma(8), dma(3, 26), dma(3, 26)] + [dma(26), dma(26)] * 2
    )
    for hx, hy in ((3, 2), (2, 4), (2, 2)):
        scratch += xy(1, p, r, hx, hy) + [vm(r, 128), vm(2, hy, 128), vm(2, 3, r, 128), vm(2, 3, 2, hy, 128)]
    vmem = pl.BlockSpec(memory_space=pltpu.VMEM)
    results = pl.pallas_call(
        functools.partial(kernel, sizes),
        out_shape=(
            jax.ShapeDtypeStruct(velocity.shape, f32),
            jax.ShapeDtypeStruct(density.shape, f32),
            jax.ShapeDtypeStruct(density.shape, f32),
        ),
        in_specs=[pl.BlockSpec(memory_space=pltpu.HBM)] * 4,
        out_specs=(vmem,) * 3,
        scratch_shapes=scratch,
        compiler_params=pltpu.CompilerParams(
            collective_id=0, has_side_effects=True, vmem_limit_bytes=32 * 1024 * 1024
        ),
    )(*[pltpu.with_memory_space_constraint(a, pltpu.HBM) for a in (velocity, density, offsets, eighths)])
    return write_out(results)


def solution(mesh):
    sizes = tuple(mesh.shape[a] for a in ("gx", "gy", "gz"))
    block = P("gx", "gy", "gz")
    stacked = P(None, "gx", "gy", "gz")
    return jax.shard_map(
        functools.partial(step, sizes),
        mesh=mesh,
        in_specs=(stacked, block, stacked, stacked),
        out_specs=(stacked, block, block),
        check_vma=False,
    )
```

```python
import functools
import math

import jax
import jax.numpy as jnp
from jax import lax
from jax.experimental import pallas as pl
from jax.experimental.pallas import tpu as pltpu
from jax.sharding import PartitionSpec as P

MESH = pl.DeviceIdType.MESH
RELAX = (6.0 / 7.0) / 6.0
HALO = 4
XY = [(-1, -1), (-1, 1), (1, -1), (1, 1), (-1, 0), (1, 0), (0, -1), (0, 1)]


def lanes(shape):
    return lax.broadcasted_iota(jnp.int32, shape, len(shape) - 1)


def roll(x, shift, axis):
    shift = shift % x.shape[axis]
    return x if shift == 0 else pltpu.roll(x, shift, axis)


def inside(sizes, me, delta):
    ok = None
    for n, i, d in zip(sizes, me, delta):
        if d:
            one = (i + d >= 0) & (i + d < n)
            ok = one if ok is None else ok & one
    return ok


class Comm:
    def __init__(self, sizes, me, sends, recv, zeros, dummy):
        self.sizes, self.me, self.sends, self.recv_sem = sizes, me, sends, recv
        self.zeros, self.dummy = zeros, dummy
        self.copies, self.rows = [], 0

    def add(self, delta, src, dst):
        device = tuple(i + d for i, d in zip(self.me, delta))
        copy = pltpu.make_async_remote_copy(
            src_ref=src, dst_ref=dst, send_sem=self.sends[len(self.copies)], recv_sem=self.recv_sem,
            device_id=device, device_id_type=MESH,
        )
        to = inside(self.sizes, self.me, delta)
        source = inside(self.sizes, self.me, tuple(-d for d in delta))
        self.copies.append((copy, to, source, dst))
        self.rows += math.prod(dst.shape) // 128

    def missing(self):
        for copy, to, source, dst in self.copies:
            zero = next(z for z in self.zeros if z.shape[2] == dst.shape[-2])
            n = dst.shape[-3] if len(dst.shape) > 2 else 1
            zero = zero.at[:, 0:n] if len(dst.shape) == 4 else zero.at[0, 0:n] if len(dst.shape) == 3 else zero.at[0, 0]

            @pl.when(jnp.logical_not(source))
            def _(dst=dst, zero=zero):
                pltpu.make_async_copy(zero, dst, self.recv_sem).start()

    def start(self):
        for copy, to, source, dst in self.copies:
            pl.when(to)(copy.start)

    def recv(self):
        all_rows = self.dummy.at[0 : self.rows]
        pltpu.make_async_copy(all_rows, all_rows, self.recv_sem).wait()

    def sent(self):
        for copy, to, source, dst in self.copies:
            pl.when(to)(copy.wait_send)


def pick(d):
    return {-1: 0, 1: 1}[d]


def cut_strips(own, strips):
    f, p, r, _ = own.shape
    hy = strips.shape[3]
    for i in range(p):
        strips[0, :, i] = own[:, i, 0:hy, :]
        strips[1, :, i] = own[:, i, r - hy : r, :]


def add_xy(comm, own, strips, bufs, dz=0, deltas=XY):
    rx, ry, rc = bufs
    p, hx = own.shape[1], rx.shape[2]
    for dx, dy in deltas:
        xs = slice(0, hx) if dx < 0 else slice(p - hx, p)
        if dy == 0:
            src, dst = own.at[:, xs], rx.at[pick(-dx)]
        elif dx == 0:
            src, dst = strips.at[pick(dy)], ry.at[pick(-dy)]
        else:
            src, dst = strips.at[pick(dy), :, xs], rc.at[pick(-dx), pick(-dy)]
        comm.add((dx, dy, dz), src, dst)


def frame_halo(bufs, p, r, out):
    rx, ry, rc = bufs
    hx, hy = rx.shape[2], ry.shape[3]
    for sx, xs in ((0, slice(HALO - hx, HALO)), (1, slice(HALO + p, HALO + p + hx))):
        out[:, xs, HALO : HALO + r, :] = rx[sx]
        for sy, ys in ((0, slice(HALO - hy, HALO)), (1, slice(HALO + r, HALO + r + hy))):
            out[:, xs, ys, :] = rc[sx, sy]
    for sy, ys in ((0, slice(HALO - hy, HALO)), (1, slice(HALO + r, HALO + r + hy))):
        out[:, HALO : HALO + p, ys, :] = ry[sy]


def swap_blocks(regs, width, shift=0):
    n = len(regs)
    lane = lanes(regs[0].shape)
    into, outof = ((lane + shift) & 127) // width, lane // width
    bits = [1 << k for k in range(n.bit_length() - 1)]
    for bit in bits:
        mask = (into & bit) != 0
        regs = [jnp.where(mask, regs[(i + bit) % n], regs[i]) for i in range(n)]
    regs = [roll(regs[i], width * i + shift, 1) for i in range(n)]
    regs = [regs[-i % n] for i in range(n)]
    for bit in bits:
        mask = (outof & bit) != 0
        regs = [jnp.where(mask, regs[(i - bit) % n], regs[i]) for i in range(n)]
    return regs


def gather(x, index):
    return jnp.take_along_axis(x, index, axis=1, mode="promise_in_bounds")


def plan_block(v, place, weight):
    lane = lanes((8, 128))
    part = (lane >> 3) & 1
    ox, oy, oz = v & 7, (v >> 3) & 7, (v >> 6) & 7
    fx = ((v >> 9) & 7).astype(jnp.float32) * 0.125
    fy = ((v >> 12) & 7).astype(jnp.float32) * 0.125
    fz = ((v >> 15) & 7).astype(jnp.float32) * 0.125
    spot = (lane & 7) + oz + part
    place[0] = ((lane >> 4) + ox) * 8 + (spot & 7)
    place[1] = spot
    wz = jnp.where(part == 0, 1.0 - fz, fz)
    for dy in range(9):
        weight[dy] = jnp.where(oy == dy, 1.0 - fy, jnp.where(oy == dy - 1, fy, 0.0))
    weight[9] = (1.0 - fx) * wz
    weight[10] = fx * wz


def advect_block(place, weight, steps, load):
    near = place[1] < 8
    result = None
    for cx in range(2):
        index = place[0] + 8 * cx
        total = None
        for dy in steps:
            value = weight[dy] * jnp.where(near, gather(load(0, dy), index), gather(load(1, dy), index))
            total = value if total is None else total + value
        total = weight[9 + cx] * total
        result = total if result is None else result + total
    return result


def kernel(sizes, vel_hbm, den_hbm, off_hbm, eig_hbm, new_vel, new_den, press, off, eig, fetch_sem, fields, stripA, rxA, ryA, rcA, mixed,
           edge, gotP, src, code, place, weight, resT, u, extU, packU, wide, s0, q0, r0,
           tmp0, own1, strip1, rx1, ry1, rc1, rz1, ext1, wide1, q1, r1, tmp1, own2, got2, ext2, sum1, fine,
           sends, recvs, z32, z16, z8, z4, z2, dummy, *bufB):
    me = tuple(lax.axis_index(a) for a in ("gx", "gy", "gz"))
    p, r = fields.shape[1], fields.shape[2]
    p1, r1n = p // 2, r // 2
    p2, r2n = p1 // 2, r1n // 2
    pairs = [(vel_hbm, fields.at[0:3]), (den_hbm, fields.at[3]), (off_hbm, off), (eig_hbm, eig)]
    fetch = [pltpu.make_async_copy(a, b, fetch_sem.at[i]) for i, (a, b) in enumerate(pairs)]
    for copy in fetch:
        copy.start()
    for zero in (z32, z16, z8, z4, z2):
        zero[...] = jnp.zeros(zero.shape, jnp.float32)

    barrier = pltpu.get_barrier_semaphore()
    peers = [(dx, dy, dz) for dz in (-1, 0, 1) for dx in (-1, 0, 1) for dy in (-1, 0, 1) if (dx, dy, dz) != (0, 0, 0)]
    count = jnp.int32(0)
    for delta in peers:
        ok = inside(sizes, me, delta)

        @pl.when(ok)
        def _():
            pl.semaphore_signal(barrier, inc=1, device_id=tuple(i + d for i, d in zip(me, delta)), device_id_type=MESH)

        count = count + jnp.where(ok, 1, 0)

    made = []
    zeros = [z32, z16, z8, z4, z2]

    def comm(at):
        sems = [sends.at[i] for i in range(at, sends.shape[0])]
        made.append(Comm(sizes, me, sems, recvs.at[len(made)], zeros, dummy))
        return made[-1]

    commA = [comm(8 * c) for c in range(4)]
    for c in range(4):
        add_xy(commA[c], fields.at[c : c + 1], stripA.at[:, c : c + 1], (rxA.at[:, c : c + 1], ryA.at[:, c : c + 1], rcA.at[:, :, c : c + 1]))
    zA = [comm(32) for c in range(4)]
    for c in range(4):
        zA[c].add((0, 0, -1), edge.at[c], gotP.at[1, c])
        zA[c].add((0, 0, 1), edge.at[c], gotP.at[0, c])
    fieldB = [bufB[8 * c : 8 * c + 8] for c in range(3)]
    commB = [comm(0) for c in range(3)]
    for c, (strip, rx, ry, rc, edgeB, estrB, ezB, ezyB) in enumerate(fieldB):
        add_xy(commB[c], u.at[c : c + 1], strip, (rx, ry, rc))
        for dz in (-1, 1):
            for dx in (-1, 1, 0):
                for dy in (-1, 1):
                    commB[c].add((dx, dy, dz), estrB.at[pick(dy)], ezyB.at[pick(-dz), 1 - dx, pick(-dy)])
                commB[c].add((dx, 0, dz), edgeB, ezB.at[pick(-dz), 1 - dx])
    commC = comm(0)
    commD = comm(0)
    for dz in (-1, 1, 0):
        add_xy(commC, own1, strip1, (rx1.at[1 - dz], ry1.at[1 - dz], rc1.at[1 - dz]), dz, XY[4:] if dz else XY)
        for dx, dy in XY[4:] if dz else XY:
            commD.add((dx, dy, dz), own2, got2.at[1 - dz, 1 - dx, 1 - dy])
        if dz:
            commC.add((0, 0, dz), own1, rz1.at[pick(-dz)])
            commD.add((0, 0, dz), own2, got2.at[1 - dz, 1, 1])
    for each in made[:8]:
        each.missing()
    for z in (0, 2):
        rc1[z] = jnp.zeros(rc1.shape[1:], jnp.float32)
        for x in (0, 2):
            for y in (0, 2):
                got2[z, x, y] = jnp.zeros(got2.shape[3:], jnp.float32)
    ext2[...] = jnp.zeros(ext2.shape, jnp.float32)
    sum1[...] = jnp.zeros(sum1.shape, jnp.float32)
    for copy in fetch[:2]:
        copy.wait()
    cut_strips(fields, stripA)
    pl.semaphore_wait(barrier, count)
    for each in commA:
        each.start()
    for each in made[8:]:
        each.missing()

    even = ((lanes((8, 128)) >> 3) & 1) == 0

    def positions():
        for copy in fetch[2:]:
            copy.wait()
        whole = (off[0] + 4) + 8 * (off[1] + 4) + 64 * (off[2] + 4)
        code[...] = whole + 512 * eig[0] + 4096 * eig[1] + 32768 * eig[2]
        for t in range(r // 8):
            for q, v in enumerate(swap_blocks([code[x, 8 * t : 8 * t + 8] for x in range(p)], 16)):
                code[q, 8 * t : 8 * t + 8] = v
        for t in range(r // 8):

            def plan(q, carry):
                v = code[q, 8 * t : 8 * t + 8]
                plan_block(jnp.where(even, v, roll(v, 8, 1)), place.at[t, 2 * q], weight.at[t, 2 * q])
                plan_block(jnp.where(even, roll(v, -8, 1), v), place.at[t, 2 * q + 1], weight.at[t, 2 * q + 1])
                return carry

            lax.fori_loop(0, 8, plan, 0)

    positions()
    rows = r + 8
    blocks = 128 // 8
    half = r // 8
    lane16 = lanes((r, 128))
    lane = lanes((rows, 128))

    def advect(c, t, b):
        totals = advect_block(place.at[t, b], weight.at[t, b], range(9), lambda far, dy: src[c, b + far, 8 * t + 4 + dy : 8 * t + 12 + dy, :])
        resT[c, t, b] = totals

    def put(c, b, start, size, v):
        if b == 0:
            edge[c, start : start + size] = v
        else:
            src[c, b, start : start + size] = v

    low = (lanes((r + 16, 128)) & 7) < 4
    for c in range(4):
        commA[c].recv()
        for t in range(half):
            ys = slice(8 * t, 8 * t + 8)
            planes = [rxA[0, c, x, ys] for x in range(HALO)] + [fields[c, x, ys] for x in range(p)] + [rxA[1, c, x, ys] for x in range(HALO)]
            for b, v in enumerate(swap_blocks(planes, 8, 4)):
                put(c, b, 8 + 8 * t, 8, v)
        for side, at in ((1, 0), (0, 4)):
            for x in range(HALO):
                mixed[c, x, at : at + 4] = rcA[0, side, c, x]
                mixed[c, HALO + p + x, at : at + 4] = rcA[1, side, c, x]
            for x in range(p):
                mixed[c, HALO + x, at : at + 4] = ryA[side, c, x]
        for b, v in enumerate(swap_blocks([mixed[c, x] for x in range(p + 8)], 8, 4)):
            put(c, b, 4, 4, v[4:8])
            put(c, b, r + 8, 4, v[0:4])
        if c:
            zA[c - 1].sent()
        zA[c].start()
        for b in range(1, blocks - 1):
            for t in range(half):
                advect(c, t, b)
        zA[c].recv()
        src[c, 0] = jnp.where(low, gotP[0, c], edge[c])
        src[c, blocks] = jnp.where(low, edge[c], gotP[1, c])
        for b in (0, blocks - 1):
            for t in range(half):
                advect(c, t, b)
        for t in range(half):
            pairs = []
            for q in range(blocks // 2):
                one, two = resT[c, t, 2 * q], resT[c, t, 2 * q + 1]
                move = jnp.where(even, two, one)
                pairs.append(jnp.where(even, one, two) + jnp.where(even, roll(move, -8, 1), roll(move, 8, 1)))
            for x, v in enumerate(swap_blocks(pairs, 16)):
                u[c, x, 8 * t : 8 * t + 8] = v
        if c == 3:
            new_den[...] = u[3]
            break
        strip, rx, ry, rc, edgeB, estrB, ezB, ezyB = fieldB[c]
        cut_strips(u.at[c : c + 1], strip)
        total = roll(u[c, 0], 4, 1)
        for x in range(1, p):
            total = jnp.where(lane16 >= 8 * x, roll(u[c, x], 4 + 8 * x, 1), total)
        edgeB[...] = total
        estrB[0] = total[0 : estrB.shape[1]]
        estrB[1] = total[r - estrB.shape[1] : r]
        for each in commB[c - 1 : c] if c else commA:
            each.sent()
        commB[c].start()

    extU[:, HALO : HALO + p, HALO : HALO + r, :] = u[0:3]
    zA[3].sent()
    commB[2].sent()
    for c in range(3):
        commB[c].recv()

    def edges(lo, hi):
        spot = lanes(lo[0].shape)
        v = [jnp.where((spot & 7) < 4, lo[i], hi[i]) for i in range(3)]
        return jnp.where(spot < 32, roll(v[0], -32, 1), jnp.where(spot < 96, roll(v[1], 32, 1), roll(v[2], 96, 1)))

    for c, (strip, rx, ry, rc, edgeB, estrB, ezB, ezyB) in enumerate(fieldB):
        frame_halo((rx, ry, rc), p, r, extU.at[c : c + 1])
        hy = estrB.shape[1]
        packU[c, HALO : HALO + r] = edges([ezB[0, i] for i in range(3)], [ezB[1, i] for i in range(3)])
        for sy, ys in ((0, slice(HALO - hy, HALO)), (1, slice(HALO + r, HALO + r + hy))):
            packU[c, ys] = edges([ezyB[0, i, sy] for i in range(3)], [ezyB[1, i, sy] for i in range(3)])
    for c in range(3):
        for x in range(HALO - 3, HALO + p + 3):
            wide[c, x, :, 0:128] = extU[c, x]
            wide[c, x, :, 128:256] = roll(packU[c], -(8 * x + 4), 1)

    def yz_mask(nrows, first_row, block_rows, cells):
        row = lax.broadcasted_iota(jnp.int32, (nrows, 256), 0) - first_row + me[1] * block_rows
        spot = lanes((nrows, 256))
        z = jnp.where(spot < 192, spot, spot - 256) + me[2] * cells
        return (row >= 0) & (row < sizes[1] * block_rows) & (z >= 0) & (z < sizes[2] * cells)

    def x_ok(x, first, block):
        g = x - first + me[0] * block
        return (g >= 0) & (g < sizes[0] * block)

    mask0 = yz_mask(rows, HALO, r, 128)

    def around(ref, x, step):
        v = ref[x]
        total = ref[x + 1] + ref[x - 1]
        total = total + roll(v, -1, 0) + roll(v, 1, 0)
        total = total + roll(v, -step, 1) + roll(v, step, 1)
        return 6.0 * v - total

    def second(ref, x, scale, step):
        v = ref[x]
        first = (RELAX * scale) * v
        return first + RELAX * (scale * v - (RELAX * scale) * around(ref, x, step))

    def source0(x, carry):
        part = wide[0, x + 1] - wide[0, x - 1]
        v = wide[1, x]
        part = part + (roll(v, -1, 0) - roll(v, 1, 0))
        v = wide[2, x]
        part = part + (roll(v, -1, 1) - roll(v, 1, 1))
        s0[x] = jnp.where(mask0 & x_ok(x, HALO, p), -0.5 * part, 0.0)
        return carry

    lax.fori_loop(HALO - 2, HALO + p + 2, source0, 0)

    def second0(x, carry):
        q0[x] = jnp.where(mask0 & x_ok(x, HALO, p), second(s0, x, 1.0, 1), 0.0)
        return carry

    lax.fori_loop(HALO - 1, HALO + p + 1, second0, 0)

    def residual0(x, carry):
        r0[x] = (s0[x] - around(q0, x, 1))[:, 0:128]
        return carry

    lax.fori_loop(HALO, HALO + p, residual0, 0)
    lane8 = lanes((r // 2, 128))
    for x in range(p // 2):
        tmp0[...] = r0[HALO + 2 * x] + r0[HALO + 2 * x + 1]
        v = tmp0[pl.ds(HALO, r // 2, stride=2), :] + tmp0[pl.ds(HALO + 1, r // 2, stride=2), :]
        v = v + jnp.where((lane8 & 1) == 0, roll(v, -1, 1), roll(v, 1, 1))
        own1[0, x] = 0.125 * v

    cut_strips(own1, strip1)
    commC.start()
    commC.sent()
    commC.recv()
    rows1 = r1n + 8
    for dz in range(3):
        ext1[dz, :, HALO : HALO + p1, HALO : HALO + r1n, :] = own1[...] if dz == 1 else rz1[dz // 2]
        frame_halo((rx1.at[dz], ry1.at[dz], rc1.at[dz]), p1, r1n, ext1.at[dz])
    lane1 = lanes((rows1, 128))
    for x in range(HALO - 2, HALO + p1 + 2):
        wide1[x, :, 0:128] = ext1[1, 0, x]
        wide1[x, :, 128:256] = jnp.where(lane1 < 64, ext1[2, 0, x], ext1[0, 0, x])
    mask1 = yz_mask(rows1, HALO, r1n, 128)
    for x in range(HALO - 1, HALO + p1 + 1):
        q1[x] = jnp.where(mask1 & x_ok(x, HALO, p1), second(wide1, x, 4.0, 2), 0.0)
    for x in range(HALO, HALO + p1):
        r1[x] = (wide1[x] - 0.25 * around(q1, x, 2))[:, 0:128]
    lane4 = lanes((r2n, 128))
    for x in range(p2):
        tmp1[...] = r1[HALO + 2 * x] + r1[HALO + 2 * x + 1]
        v = tmp1[pl.ds(HALO, r2n, stride=2), :] + tmp1[pl.ds(HALO + 1, r2n, stride=2), :]
        v = v + jnp.where((lane4 & 3) < 2, roll(v, -2, 1), roll(v, 2, 1))
        own2[x] = 0.125 * v

    commD.start()
    got2[1, 1, 1] = own2[...]
    commD.sent()
    commD.recv()
    for z in range(3):
        for a in range(3):
            for b in range(3):
                ext2[z, p2 * a : p2 * a + p2, r2n * b : r2n * b + r2n, :] = got2[z, a, b]
    lane2 = lanes((16, 128))
    mask2 = yz_mask(16, r2n, r2n, 128)
    planes2 = {}
    for x in range(p2 - 2, 2 * p2 + 2):
        planes2[x] = jnp.concatenate([ext2[1, x], jnp.where(lane2 < 64, ext2[2, x], ext2[0, x])], axis=1)
    for x in range(p2 - 1, 2 * p2 + 1):
        v = jnp.where(mask2 & x_ok(x, p2, p2), second(planes2, x, 16.0, 4), 0.0)
        first_row = r2n - 1
        take = r2n + 2
        base = HALO - 2
        for side in range(2):
            part = v[first_row : first_row + take, 128 * side : 128 * side + 128]
            sum1[x, side, pl.ds(base, take, stride=2), :] = part
            sum1[x, side, pl.ds(base + 1, take, stride=2), :] = part
    for x1 in range(HALO - 1, HALO + p1 + 1):
        x2 = (x1 - HALO) // 2 + p2
        for side in range(2):
            v = q1[x1, :, 128 * side : 128 * side + 128] + sum1[x2, side]
            part = v[HALO - 2 : HALO - 2 + r1n + 4]
            fine[x1, side, pl.ds(0, r1n + 4, stride=2), :] = part
            fine[x1, side, pl.ds(1, r1n + 4, stride=2), :] = part
    for x in range(HALO - 1, HALO + p + 1):
        x1 = (x - HALO) // 2 + HALO
        coarse = jnp.concatenate([fine[x1, 0], fine[x1, 1]], axis=1)
        s0[x] = jnp.where(mask0 & x_ok(x, HALO, p), q0[x] + coarse, 0.0)
    for x in range(p):
        v = s0[x + HALO]
        cut = lambda t: t[HALO : HALO + r, 0:128]
        press[x] = cut(v)
        new_vel[0, x] = u[0, x] - 0.5 * cut(s0[x + HALO + 1] - s0[x + HALO - 1])
        new_vel[1, x] = u[1, x] - 0.5 * cut(roll(v, -1, 0) - roll(v, 1, 0))
        new_vel[2, x] = u[2, x] - 0.5 * cut(roll(v, -1, 1) - roll(v, 1, 1))


def write_kernel(*refs):
    n = len(refs) // 2
    copies = [pltpu.make_async_copy(refs[i], refs[n + i], refs[-1].at[i]) for i in range(n)]
    for copy in copies:
        copy.start()
    for copy in copies:
        copy.wait()


def write_out(results):
    return pl.pallas_call(
        write_kernel,
        out_shape=tuple(jax.ShapeDtypeStruct(a.shape, a.dtype) for a in results),
        in_specs=[pl.BlockSpec(memory_space=pltpu.VMEM)] * len(results),
        out_specs=(pl.BlockSpec(memory_space=pltpu.HBM),) * len(results),
        scratch_shapes=[pltpu.SemaphoreType.DMA((len(results),))],
        compiler_params=pltpu.CompilerParams(vmem_limit_bytes=1 << 20),
    )(*results)


def step(sizes, velocity, density, offsets, eighths):
    p, r, _ = density.shape
    f32 = jnp.float32

    def vm(*shape):
        return pltpu.VMEM(shape, f32)

    def xy(f, p, r, hx, hy):
        return [vm(2, f, p, hy, 128), vm(2, f, hx, r, 128), vm(2, f, p, hy, 128), vm(2, 2, f, hx, hy, 128)]

    assert p == 8 and r % 8 == 0
    p1, r1, p2, r2 = p // 2, r // 2, p // 4, r // 4
    rows, rows1 = r + 8, r1 + 8
    dma = lambda *n: pltpu.SemaphoreType.DMA(n)
    half = r // 8
    scratch = (
        [pltpu.VMEM(offsets.shape, jnp.int32), pltpu.VMEM(eighths.shape, jnp.int32), dma(4), vm(4, p, r, 128)] + xy(4, p, r, 4, 4)
        + [vm(4, p + 8, 8, 128), vm(4, r + 16, 128), vm(2, 4, r + 16, 128), vm(4, 17, r + 16, 128),
           pltpu.VMEM((p, r, 128), jnp.int32), pltpu.VMEM((half, 16, 2, 8, 128), jnp.int32), vm(half, 16, 11, 8, 128),
           vm(4, half, 16, 8, 128), vm(4, p, r, 128)]
        + [vm(3, p + 8, rows, 128), vm(3, rows, 128), vm(3, p + 8, rows, 256),
           vm(p + 8, rows, 256), vm(p + 8, rows, 256), vm(p + 8, rows, 128), vm(rows, 128), vm(1, p1, r1, 128)]
        + [vm(2, 1, p1, 2, 128), vm(3, 2, 1, 2, r1, 128), vm(3, 2, 1, p1, 2, 128), vm(3, 2, 2, 1, 2, 2, 128), vm(2, 1, p1, r1, 128)]
        + [vm(3, 1, p1 + 8, rows1, 128), vm(p1 + 8, rows1, 256), vm(p1 + 8, rows1, 256),
           vm(p1 + 8, rows1, 128), vm(rows1, 128), vm(p2, r2, 128), vm(3, 3, 3, p2, r2, 128), vm(3, 3 * p2, 16, 128),
           vm(3 * p2, 2, rows1, 128), vm(p1 + 8, 2, rows, 128)]
        + [dma(34), dma(13), vm(1, 1, r + 16, 128), vm(1, 4, r, 128), vm(1, 4, 8, 128), vm(1, 8, 4, 128), vm(1, 8, 2, 128), vm(512, 128)]
    )
    for hx, hy in ((3, 2), (2, 4), (2, 2)):
        scratch += xy(1, p, r, hx, hy) + [vm(r, 128), vm(2, hy, 128), vm(2, 3, r, 128), vm(2, 3, 2, hy, 128)]
    vmem = pl.BlockSpec(memory_space=pltpu.VMEM)
    results = pl.pallas_call(
        functools.partial(kernel, sizes),
        out_shape=(
            jax.ShapeDtypeStruct(velocity.shape, f32),
            jax.ShapeDtypeStruct(density.shape, f32),
            jax.ShapeDtypeStruct(density.shape, f32),
        ),
        in_specs=[pl.BlockSpec(memory_space=pltpu.HBM)] * 4,
        out_specs=(vmem,) * 3,
        scratch_shapes=scratch,
        compiler_params=pltpu.CompilerParams(
            collective_id=0, has_side_effects=True, vmem_limit_bytes=32 * 1024 * 1024
        ),
    )(*[pltpu.with_memory_space_constraint(a, pltpu.HBM) for a in (velocity, density, offsets, eighths)])
    return write_out(results)


def solution(mesh):
    sizes = tuple(mesh.shape[a] for a in ("gx", "gy", "gz"))
    block = P("gx", "gy", "gz")
    stacked = P(None, "gx", "gy", "gz")
    return jax.shard_map(
        functools.partial(step, sizes),
        mesh=mesh,
        in_specs=(stacked, block, stacked, stacked),
        out_specs=(stacked, block, block),
        check_vma=False,
    )
```

```python
import functools
import math

import jax
import jax.numpy as jnp
from jax import lax
from jax.experimental import pallas as pl
from jax.experimental.pallas import tpu as pltpu
from jax.sharding import PartitionSpec as P

MESH = pl.DeviceIdType.MESH
RELAX = (6.0 / 7.0) / 6.0
HALO = 4
XY = [(-1, -1), (-1, 1), (1, -1), (1, 1), (-1, 0), (1, 0), (0, -1), (0, 1)]


def lanes(shape):
    return lax.broadcasted_iota(jnp.int32, shape, len(shape) - 1)


def roll(x, shift, axis):
    shift = shift % x.shape[axis]
    return x if shift == 0 else pltpu.roll(x, shift, axis)


def inside(sizes, me, delta):
    ok = None
    for n, i, d in zip(sizes, me, delta):
        if d:
            one = (i + d >= 0) & (i + d < n)
            ok = one if ok is None else ok & one
    return ok


class Comm:
    def __init__(self, sizes, me, sends, recv, zeros, dummy):
        self.sizes, self.me, self.sends, self.recv_sem = sizes, me, sends, recv
        self.zeros, self.dummy = zeros, dummy
        self.copies, self.rows = [], 0

    def add(self, delta, src, dst):
        device = tuple(i + d for i, d in zip(self.me, delta))
        copy = pltpu.make_async_remote_copy(
            src_ref=src, dst_ref=dst, send_sem=self.sends[len(self.copies)], recv_sem=self.recv_sem,
            device_id=device, device_id_type=MESH,
        )
        to = inside(self.sizes, self.me, delta)
        source = inside(self.sizes, self.me, tuple(-d for d in delta))
        self.copies.append((copy, to, source, dst))
        self.rows += math.prod(dst.shape) // 128

    def missing(self):
        for copy, to, source, dst in self.copies:
            zero = next(z for z in self.zeros if z.shape[2] == dst.shape[-2])
            n = dst.shape[-3] if len(dst.shape) > 2 else 1
            zero = zero.at[:, 0:n] if len(dst.shape) == 4 else zero.at[0, 0:n] if len(dst.shape) == 3 else zero.at[0, 0]

            @pl.when(jnp.logical_not(source))
            def _(dst=dst, zero=zero):
                pltpu.make_async_copy(zero, dst, self.recv_sem).start()

    def start(self):
        for copy, to, source, dst in self.copies:
            pl.when(to)(copy.start)

    def recv(self):
        all_rows = self.dummy.at[0 : self.rows]
        pltpu.make_async_copy(all_rows, all_rows, self.recv_sem).wait()

    def sent(self):
        for copy, to, source, dst in self.copies:
            pl.when(to)(copy.wait_send)


def pick(d):
    return {-1: 0, 1: 1}[d]


def cut_strips(own, strips):
    f, p, r, _ = own.shape
    hy = strips.shape[3]
    for i in range(p):
        strips[0, :, i] = own[:, i, 0:hy, :]
        strips[1, :, i] = own[:, i, r - hy : r, :]


def add_xy(comm, own, strips, bufs, dz=0, deltas=XY):
    rx, ry, rc = bufs
    p, hx = own.shape[1], rx.shape[2]
    for dx, dy in deltas:
        xs = slice(0, hx) if dx < 0 else slice(p - hx, p)
        if dy == 0:
            src, dst = own.at[:, xs], rx.at[pick(-dx)]
        elif dx == 0:
            src, dst = strips.at[pick(dy)], ry.at[pick(-dy)]
        else:
            src, dst = strips.at[pick(dy), :, xs], rc.at[pick(-dx), pick(-dy)]
        comm.add((dx, dy, dz), src, dst)


def frame_halo(bufs, p, r, out):
    rx, ry, rc = bufs
    hx, hy = rx.shape[2], ry.shape[3]
    for sx, xs in ((0, slice(HALO - hx, HALO)), (1, slice(HALO + p, HALO + p + hx))):
        out[:, xs, HALO : HALO + r, :] = rx[sx]
        for sy, ys in ((0, slice(HALO - hy, HALO)), (1, slice(HALO + r, HALO + r + hy))):
            out[:, xs, ys, :] = rc[sx, sy]
    for sy, ys in ((0, slice(HALO - hy, HALO)), (1, slice(HALO + r, HALO + r + hy))):
        out[:, HALO : HALO + p, ys, :] = ry[sy]


def swap_blocks(regs, width, shift=0):
    n = len(regs)
    lane = lanes(regs[0].shape)
    into, outof = ((lane + shift) & 127) // width, lane // width
    bits = [1 << k for k in range(n.bit_length() - 1)]
    for bit in bits:
        mask = (into & bit) != 0
        regs = [jnp.where(mask, regs[(i + bit) % n], regs[i]) for i in range(n)]
    regs = [roll(regs[i], width * i + shift, 1) for i in range(n)]
    regs = [regs[-i % n] for i in range(n)]
    for bit in bits:
        mask = (outof & bit) != 0
        regs = [jnp.where(mask, regs[(i - bit) % n], regs[i]) for i in range(n)]
    return regs


def gather(x, index):
    return jnp.take_along_axis(x, index, axis=1, mode="promise_in_bounds")


def plan_block(v, place, weight):
    lane = lanes((8, 128))
    part = (lane >> 3) & 1
    ox, oy, oz = v & 7, (v >> 3) & 7, (v >> 6) & 7
    fx = ((v >> 9) & 7).astype(jnp.float32) * 0.125
    fy = ((v >> 12) & 7).astype(jnp.float32) * 0.125
    fz = ((v >> 15) & 7).astype(jnp.float32) * 0.125
    spot = (lane & 7) + oz + part
    place[0] = ((lane >> 4) + ox) * 8 + (spot & 7)
    place[1] = spot
    wz = jnp.where(part == 0, 1.0 - fz, fz)
    for dy in range(9):
        weight[dy] = jnp.where(oy == dy, 1.0 - fy, jnp.where(oy == dy - 1, fy, 0.0))
    weight[9] = (1.0 - fx) * wz
    weight[10] = fx * wz


def advect_block(place, weight, steps, load):
    near = place[1] < 8
    result = None
    for cx in range(2):
        index = place[0] + 8 * cx
        total = None
        for dy in steps:
            value = weight[dy] * jnp.where(near, gather(load(0, dy), index), gather(load(1, dy), index))
            total = value if total is None else total + value
        total = weight[9 + cx] * total
        result = total if result is None else result + total
    return result


def kernel(sizes, vel_hbm, den_hbm, off_hbm, eig_hbm, new_vel, new_den, press, off, eig, fetch_sem, fields, stripA, rxA, ryA, rcA, mixed,
           edge, gotP, src, code, place, weight, resT, u, extU, packU, wide, s0, q0, r0,
           tmp0, own1, strip1, rx1, ry1, rc1, rz1, ext1, wide1, q1, r1, tmp1, own2, got2, ext2, sum1, fine,
           sends, recvs, z32, z16, z8, z4, z2, dummy, *bufB):
    me = tuple(lax.axis_index(a) for a in ("gx", "gy", "gz"))
    p, r = fields.shape[1], fields.shape[2]
    p1, r1n = p // 2, r // 2
    p2, r2n = p1 // 2, r1n // 2
    pairs = [(vel_hbm, fields.at[0:3]), (den_hbm, fields.at[3]), (off_hbm, off), (eig_hbm, eig)]
    fetch = [pltpu.make_async_copy(a, b, fetch_sem.at[i]) for i, (a, b) in enumerate(pairs)]
    for copy in fetch:
        copy.start()
    barrier = pltpu.get_barrier_semaphore()
    peers = [(dx, dy, dz) for dz in (-1, 0, 1) for dx in (-1, 0, 1) for dy in (-1, 0, 1) if (dx, dy, dz) != (0, 0, 0)]
    count = jnp.int32(0)
    for delta in peers:
        ok = inside(sizes, me, delta)

        @pl.when(ok)
        def _():
            pl.semaphore_signal(barrier, inc=1, device_id=tuple(i + d for i, d in zip(me, delta)), device_id_type=MESH)

        count = count + jnp.where(ok, 1, 0)

    for zero in (z32, z16, z8, z4, z2):
        zero[...] = jnp.zeros(zero.shape, jnp.float32)
    made = []
    zeros = [z32, z16, z8, z4, z2]

    def comm(at):
        sems = [sends.at[i] for i in range(at, sends.shape[0])]
        made.append(Comm(sizes, me, sems, recvs.at[len(made)], zeros, dummy))
        return made[-1]

    commA = [comm(8 * c) for c in range(4)]
    for c in range(4):
        add_xy(commA[c], fields.at[c : c + 1], stripA.at[:, c : c + 1], (rxA.at[:, c : c + 1], ryA.at[:, c : c + 1], rcA.at[:, :, c : c + 1]))
    zA = [comm(32) for c in range(4)]
    for c in range(4):
        zA[c].add((0, 0, -1), edge.at[c], gotP.at[1, c])
        zA[c].add((0, 0, 1), edge.at[c], gotP.at[0, c])
    fieldB = [bufB[8 * c : 8 * c + 8] for c in range(3)]
    commB = [comm(0) for c in range(3)]
    for c, (strip, rx, ry, rc, edgeB, estrB, ezB, ezyB) in enumerate(fieldB):
        add_xy(commB[c], u.at[c : c + 1], strip, (rx, ry, rc))
        for dz in (-1, 1):
            for dx in (-1, 1, 0):
                for dy in (-1, 1):
                    commB[c].add((dx, dy, dz), estrB.at[pick(dy)], ezyB.at[pick(-dz), 1 - dx, pick(-dy)])
                commB[c].add((dx, 0, dz), edgeB, ezB.at[pick(-dz), 1 - dx])
    commC = comm(0)
    commD = comm(0)
    for dz in (-1, 1, 0):
        add_xy(commC, own1, strip1, (rx1.at[1 - dz], ry1.at[1 - dz], rc1.at[1 - dz]), dz, XY[4:] if dz else XY)
        for dx, dy in XY[4:] if dz else XY:
            commD.add((dx, dy, dz), own2, got2.at[1 - dz, 1 - dx, 1 - dy])
        if dz:
            commC.add((0, 0, dz), own1, rz1.at[pick(-dz)])
            commD.add((0, 0, dz), own2, got2.at[1 - dz, 1, 1])
    for each in made[:8]:
        each.missing()
    for z in (0, 2):
        rc1[z] = jnp.zeros(rc1.shape[1:], jnp.float32)
        for x in (0, 2):
            for y in (0, 2):
                got2[z, x, y] = jnp.zeros(got2.shape[3:], jnp.float32)
    ext2[...] = jnp.zeros(ext2.shape, jnp.float32)
    sum1[...] = jnp.zeros(sum1.shape, jnp.float32)
    for copy in fetch[:2]:
        copy.wait()
    cut_strips(fields, stripA)
    pl.semaphore_wait(barrier, count)
    for each in commA:
        each.start()
    for each in made[8:]:
        each.missing()

    even = ((lanes((8, 128)) >> 3) & 1) == 0

    def positions():
        for copy in fetch[2:]:
            copy.wait()
        whole = (off[0] + 4) + 8 * (off[1] + 4) + 64 * (off[2] + 4)
        code[...] = whole + 512 * eig[0] + 4096 * eig[1] + 32768 * eig[2]
        for t in range(r // 8):
            for q, v in enumerate(swap_blocks([code[x, 8 * t : 8 * t + 8] for x in range(p)], 16)):
                code[q, 8 * t : 8 * t + 8] = v
        for t in range(r // 8):

            def plan(q, carry):
                v = code[q, 8 * t : 8 * t + 8]
                plan_block(jnp.where(even, v, roll(v, 8, 1)), place.at[t, 2 * q], weight.at[t, 2 * q])
                plan_block(jnp.where(even, roll(v, -8, 1), v), place.at[t, 2 * q + 1], weight.at[t, 2 * q + 1])
                return carry

            lax.fori_loop(0, 8, plan, 0)

    positions()
    rows = r + 8
    blocks = 128 // 8
    half = r // 8
    lane16 = lanes((r, 128))
    lane = lanes((rows, 128))

    def advect(c, t, b):
        totals = advect_block(place.at[t, b], weight.at[t, b], range(9), lambda far, dy: src[c, b + far, 8 * t + 4 + dy : 8 * t + 12 + dy, :])
        resT[c, t, b] = totals

    def put(c, b, start, size, v):
        if b == 0:
            edge[c, start : start + size] = v
        else:
            src[c, b, start : start + size] = v

    low = (lanes((r + 16, 128)) & 7) < 4
    for c in range(4):
        commA[c].recv()
        for t in range(half):
            ys = slice(8 * t, 8 * t + 8)
            planes = [rxA[0, c, x, ys] for x in range(HALO)] + [fields[c, x, ys] for x in range(p)] + [rxA[1, c, x, ys] for x in range(HALO)]
            for b, v in enumerate(swap_blocks(planes, 8, 4)):
                put(c, b, 8 + 8 * t, 8, v)
        for side, at in ((1, 0), (0, 4)):
            for x in range(HALO):
                mixed[c, x, at : at + 4] = rcA[0, side, c, x]
                mixed[c, HALO + p + x, at : at + 4] = rcA[1, side, c, x]
            for x in range(p):
                mixed[c, HALO + x, at : at + 4] = ryA[side, c, x]
        for b, v in enumerate(swap_blocks([mixed[c, x] for x in range(p + 8)], 8, 4)):
            put(c, b, 4, 4, v[4:8])
            put(c, b, r + 8, 4, v[0:4])
        if c:
            zA[c - 1].sent()
        zA[c].start()
        for b in range(1, blocks - 1):
            for t in range(half):
                advect(c, t, b)
        zA[c].recv()
        src[c, 0] = jnp.where(low, gotP[0, c], edge[c])
        src[c, blocks] = jnp.where(low, edge[c], gotP[1, c])
        for b in (0, blocks - 1):
            for t in range(half):
                advect(c, t, b)
        for t in range(half):
            pairs = []
            for q in range(blocks // 2):
                one, two = resT[c, t, 2 * q], resT[c, t, 2 * q + 1]
                move = jnp.where(even, two, one)
                pairs.append(jnp.where(even, one, two) + jnp.where(even, roll(move, -8, 1), roll(move, 8, 1)))
            for x, v in enumerate(swap_blocks(pairs, 16)):
                u[c, x, 8 * t : 8 * t + 8] = v
        if c == 3:
            new_den[...] = u[3]
            break
        strip, rx, ry, rc, edgeB, estrB, ezB, ezyB = fieldB[c]
        cut_strips(u.at[c : c + 1], strip)
        total = roll(u[c, 0], 4, 1)
        for x in range(1, p):
            total = jnp.where(lane16 >= 8 * x, roll(u[c, x], 4 + 8 * x, 1), total)
        edgeB[...] = total
        estrB[0] = total[0 : estrB.shape[1]]
        estrB[1] = total[r - estrB.shape[1] : r]
        for each in commB[c - 1 : c] if c else commA:
            each.sent()
        commB[c].start()

    extU[:, HALO : HALO + p, HALO : HALO + r, :] = u[0:3]
    zA[3].sent()
    commB[2].sent()

    def edges(lo, hi):
        spot = lanes(lo[0].shape)
        v = [jnp.where((spot & 7) < 4, lo[i], hi[i]) for i in range(3)]
        return jnp.where(spot < 32, roll(v[0], -32, 1), jnp.where(spot < 96, roll(v[1], 32, 1), roll(v[2], 96, 1)))

    def yz_mask(nrows, first_row, block_rows, cells):
        row = lax.broadcasted_iota(jnp.int32, (nrows, 256), 0) - first_row + me[1] * block_rows
        spot = lanes((nrows, 256))
        z = jnp.where(spot < 192, spot, spot - 256) + me[2] * cells
        return (row >= 0) & (row < sizes[1] * block_rows) & (z >= 0) & (z < sizes[2] * cells)

    def x_ok(x, first, block):
        g = x - first + me[0] * block
        return (g >= 0) & (g < sizes[0] * block)

    mask0 = yz_mask(rows, HALO, r, 128)

    def around(ref, x, step):
        v = ref[x]
        total = ref[x + 1] + ref[x - 1]
        total = total + roll(v, -1, 0) + roll(v, 1, 0)
        total = total + roll(v, -step, 1) + roll(v, step, 1)
        return 6.0 * v - total

    def second(ref, x, scale, step):
        v = ref[x]
        first = (RELAX * scale) * v
        return first + RELAX * (scale * v - (RELAX * scale) * around(ref, x, step))

    for c, (strip, rx, ry, rc, edgeB, estrB, ezB, ezyB) in enumerate(fieldB):
        commB[c].recv()
        frame_halo((rx, ry, rc), p, r, extU.at[c : c + 1])
        hy = estrB.shape[1]
        packU[c, HALO : HALO + r] = edges([ezB[0, i] for i in range(3)], [ezB[1, i] for i in range(3)])
        for sy, ys in ((0, slice(HALO - hy, HALO)), (1, slice(HALO + r, HALO + r + hy))):
            packU[c, ys] = edges([ezyB[0, i, sy] for i in range(3)], [ezyB[1, i, sy] for i in range(3)])
        side = packU[c]
        for x in range(HALO - 3, HALO + p + 3):
            wide[c, x, :, 0:128] = extU[c, x]
            wide[c, x, :, 128:256] = roll(side, -(8 * x + 4), 1)
        for x in range(HALO - 2, HALO + p + 2):
            if c == 0:
                s0[x] = wide[0, x + 1] - wide[0, x - 1]
            elif c == 1:
                v = wide[1, x]
                s0[x] = s0[x] + (roll(v, -1, 0) - roll(v, 1, 0))
            else:
                v = wide[2, x]
                part = s0[x] + (roll(v, -1, 1) - roll(v, 1, 1))
                s0[x] = jnp.where(mask0 & x_ok(x, HALO, p), -0.5 * part, 0.0)

    for x in range(HALO - 1, HALO + p + 1):
        q0[x] = jnp.where(mask0 & x_ok(x, HALO, p), second(s0, x, 1.0, 1), 0.0)
    for x in range(HALO, HALO + p):
        r0[x] = (s0[x] - around(q0, x, 1))[:, 0:128]
    lane8 = lanes((r // 2, 128))
    for x in range(p // 2):
        tmp0[...] = r0[HALO + 2 * x] + r0[HALO + 2 * x + 1]
        v = tmp0[pl.ds(HALO, r // 2, stride=2), :] + tmp0[pl.ds(HALO + 1, r // 2, stride=2), :]
        v = v + jnp.where((lane8 & 1) == 0, roll(v, -1, 1), roll(v, 1, 1))
        own1[0, x] = 0.125 * v

    cut_strips(own1, strip1)
    commC.start()
    commC.sent()
    commC.recv()
    rows1 = r1n + 8
    for dz in range(3):
        ext1[dz, :, HALO : HALO + p1, HALO : HALO + r1n, :] = own1[...] if dz == 1 else rz1[dz // 2]
        frame_halo((rx1.at[dz], ry1.at[dz], rc1.at[dz]), p1, r1n, ext1.at[dz])
    lane1 = lanes((rows1, 128))
    for x in range(HALO - 2, HALO + p1 + 2):
        wide1[x, :, 0:128] = ext1[1, 0, x]
        wide1[x, :, 128:256] = jnp.where(lane1 < 64, ext1[2, 0, x], ext1[0, 0, x])
    mask1 = yz_mask(rows1, HALO, r1n, 128)
    for x in range(HALO - 1, HALO + p1 + 1):
        q1[x] = jnp.where(mask1 & x_ok(x, HALO, p1), second(wide1, x, 4.0, 2), 0.0)
    for x in range(HALO, HALO + p1):
        r1[x] = (wide1[x] - 0.25 * around(q1, x, 2))[:, 0:128]
    lane4 = lanes((r2n, 128))
    for x in range(p2):
        tmp1[...] = r1[HALO + 2 * x] + r1[HALO + 2 * x + 1]
        v = tmp1[pl.ds(HALO, r2n, stride=2), :] + tmp1[pl.ds(HALO + 1, r2n, stride=2), :]
        v = v + jnp.where((lane4 & 3) < 2, roll(v, -2, 1), roll(v, 2, 1))
        own2[x] = 0.125 * v

    commD.start()
    got2[1, 1, 1] = own2[...]
    commD.sent()
    commD.recv()
    for z in range(3):
        for a in range(3):
            for b in range(3):
                ext2[z, p2 * a : p2 * a + p2, r2n * b : r2n * b + r2n, :] = got2[z, a, b]
    lane2 = lanes((16, 128))
    mask2 = yz_mask(16, r2n, r2n, 128)
    planes2 = {}
    for x in range(p2 - 2, 2 * p2 + 2):
        planes2[x] = jnp.concatenate([ext2[1, x], jnp.where(lane2 < 64, ext2[2, x], ext2[0, x])], axis=1)
    for x in range(p2 - 1, 2 * p2 + 1):
        v = jnp.where(mask2 & x_ok(x, p2, p2), second(planes2, x, 16.0, 4), 0.0)
        first_row = r2n - 1
        take = r2n + 2
        base = HALO - 2
        for side in range(2):
            part = v[first_row : first_row + take, 128 * side : 128 * side + 128]
            sum1[x, side, pl.ds(base, take, stride=2), :] = part
            sum1[x, side, pl.ds(base + 1, take, stride=2), :] = part
    for x1 in range(HALO - 1, HALO + p1 + 1):
        x2 = (x1 - HALO) // 2 + p2
        for side in range(2):
            v = q1[x1, :, 128 * side : 128 * side + 128] + sum1[x2, side]
            part = v[HALO - 2 : HALO - 2 + r1n + 4]
            fine[x1, side, pl.ds(0, r1n + 4, stride=2), :] = part
            fine[x1, side, pl.ds(1, r1n + 4, stride=2), :] = part
    for x in range(HALO - 1, HALO + p + 1):
        x1 = (x - HALO) // 2 + HALO
        coarse = jnp.concatenate([fine[x1, 0], fine[x1, 1]], axis=1)
        s0[x] = jnp.where(mask0 & x_ok(x, HALO, p), q0[x] + coarse, 0.0)
    for x in range(p):
        v = s0[x + HALO]
        cut = lambda t: t[HALO : HALO + r, 0:128]
        press[x] = cut(v)
        new_vel[0, x] = u[0, x] - 0.5 * cut(s0[x + HALO + 1] - s0[x + HALO - 1])
        new_vel[1, x] = u[1, x] - 0.5 * cut(roll(v, -1, 0) - roll(v, 1, 0))
        new_vel[2, x] = u[2, x] - 0.5 * cut(roll(v, -1, 1) - roll(v, 1, 1))


def write_kernel(*refs):
    n = len(refs) // 2
    copies = [pltpu.make_async_copy(refs[i], refs[n + i], refs[-1].at[i]) for i in range(n)]
    for copy in copies:
        copy.start()
    for copy in copies:
        copy.wait()


def write_out(results):
    return pl.pallas_call(
        write_kernel,
        out_shape=tuple(jax.ShapeDtypeStruct(a.shape, a.dtype) for a in results),
        in_specs=[pl.BlockSpec(memory_space=pltpu.VMEM)] * len(results),
        out_specs=(pl.BlockSpec(memory_space=pltpu.HBM),) * len(results),
        scratch_shapes=[pltpu.SemaphoreType.DMA((len(results),))],
        compiler_params=pltpu.CompilerParams(vmem_limit_bytes=1 << 20),
    )(*results)


def step(sizes, velocity, density, offsets, eighths):
    p, r, _ = density.shape
    f32 = jnp.float32

    def vm(*shape):
        return pltpu.VMEM(shape, f32)

    def xy(f, p, r, hx, hy):
        return [vm(2, f, p, hy, 128), vm(2, f, hx, r, 128), vm(2, f, p, hy, 128), vm(2, 2, f, hx, hy, 128)]

    assert p == 8 and r % 8 == 0
    p1, r1, p2, r2 = p // 2, r // 2, p // 4, r // 4
    rows, rows1 = r + 8, r1 + 8
    dma = lambda *n: pltpu.SemaphoreType.DMA(n)
    half = r // 8
    scratch = (
        [pltpu.VMEM(offsets.shape, jnp.int32), pltpu.VMEM(eighths.shape, jnp.int32), dma(4), vm(4, p, r, 128)] + xy(4, p, r, 4, 4)
        + [vm(4, p + 8, 8, 128), vm(4, r + 16, 128), vm(2, 4, r + 16, 128), vm(4, 17, r + 16, 128),
           pltpu.VMEM((p, r, 128), jnp.int32), pltpu.VMEM((half, 16, 2, 8, 128), jnp.int32), vm(half, 16, 11, 8, 128),
           vm(4, half, 16, 8, 128), vm(4, p, r, 128)]
        + [vm(3, p + 8, rows, 128), vm(3, rows, 128), vm(3, p + 8, rows, 256),
           vm(p + 8, rows, 256), vm(p + 8, rows, 256), vm(p + 8, rows, 128), vm(rows, 128), vm(1, p1, r1, 128)]
        + [vm(2, 1, p1, 2, 128), vm(3, 2, 1, 2, r1, 128), vm(3, 2, 1, p1, 2, 128), vm(3, 2, 2, 1, 2, 2, 128), vm(2, 1, p1, r1, 128)]
        + [vm(3, 1, p1 + 8, rows1, 128), vm(p1 + 8, rows1, 256), vm(p1 + 8, rows1, 256),
           vm(p1 + 8, rows1, 128), vm(rows1, 128), vm(p2, r2, 128), vm(3, 3, 3, p2, r2, 128), vm(3, 3 * p2, 16, 128),
           vm(3 * p2, 2, rows1, 128), vm(p1 + 8, 2, rows, 128)]
        + [dma(34), dma(13), vm(1, 1, r + 16, 128), vm(1, 4, r, 128), vm(1, 4, 8, 128), vm(1, 8, 4, 128), vm(1, 8, 2, 128), vm(512, 128)]
    )
    for hx, hy in ((3, 2), (2, 4), (2, 2)):
        scratch += xy(1, p, r, hx, hy) + [vm(r, 128), vm(2, hy, 128), vm(2, 3, r, 128), vm(2, 3, 2, hy, 128)]
    vmem = pl.BlockSpec(memory_space=pltpu.VMEM)
    results = pl.pallas_call(
        functools.partial(kernel, sizes),
        out_shape=(
            jax.ShapeDtypeStruct(velocity.shape, f32),
            jax.ShapeDtypeStruct(density.shape, f32),
            jax.ShapeDtypeStruct(density.shape, f32),
        ),
        in_specs=[pl.BlockSpec(memory_space=pltpu.HBM)] * 4,
        out_specs=(vmem,) * 3,
        scratch_shapes=scratch,
        compiler_params=pltpu.CompilerParams(
            collective_id=0, has_side_effects=True, vmem_limit_bytes=32 * 1024 * 1024
        ),
    )(*[pltpu.with_memory_space_constraint(a, pltpu.HBM) for a in (velocity, density, offsets, eighths)])
    return write_out(results)


def solution(mesh):
    sizes = tuple(mesh.shape[a] for a in ("gx", "gy", "gz"))
    block = P("gx", "gy", "gz")
    stacked = P(None, "gx", "gy", "gz")
    return jax.shard_map(
        functools.partial(step, sizes),
        mesh=mesh,
        in_specs=(stacked, block, stacked, stacked),
        out_specs=(stacked, block, block),
        check_vma=False,
    )
```

```python
import functools
import math

import jax
import jax.numpy as jnp
from jax import lax
from jax.experimental import pallas as pl
from jax.experimental.pallas import tpu as pltpu
from jax.sharding import PartitionSpec as P

MESH = pl.DeviceIdType.MESH
RELAX = (6.0 / 7.0) / 6.0
HALO = 4
XY = [(-1, -1), (-1, 1), (1, -1), (1, 1), (-1, 0), (1, 0), (0, -1), (0, 1)]


def lanes(shape):
    return lax.broadcasted_iota(jnp.int32, shape, len(shape) - 1)


def roll(x, shift, axis):
    shift = shift % x.shape[axis]
    return x if shift == 0 else pltpu.roll(x, shift, axis)


def inside(sizes, me, delta):
    ok = None
    for n, i, d in zip(sizes, me, delta):
        if d:
            one = (i + d >= 0) & (i + d < n)
            ok = one if ok is None else ok & one
    return ok


class Comm:
    def __init__(self, sizes, me, sends, recv, zeros, dummy):
        self.sizes, self.me, self.sends, self.recv_sem = sizes, me, sends, recv
        self.zeros, self.dummy = zeros, dummy
        self.copies, self.rows = [], 0

    def add(self, delta, src, dst):
        device = tuple(i + d for i, d in zip(self.me, delta))
        copy = pltpu.make_async_remote_copy(
            src_ref=src, dst_ref=dst, send_sem=self.sends[len(self.copies)], recv_sem=self.recv_sem,
            device_id=device, device_id_type=MESH,
        )
        to = inside(self.sizes, self.me, delta)
        source = inside(self.sizes, self.me, tuple(-d for d in delta))
        self.copies.append((copy, to, source, dst))
        self.rows += math.prod(dst.shape) // 128

    def missing(self):
        for copy, to, source, dst in self.copies:
            zero = next(z for z in self.zeros if z.shape[2] == dst.shape[-2])
            n = dst.shape[-3] if len(dst.shape) > 2 else 1
            zero = zero.at[:, 0:n] if len(dst.shape) == 4 else zero.at[0, 0:n] if len(dst.shape) == 3 else zero.at[0, 0]

            @pl.when(jnp.logical_not(source))
            def _(dst=dst, zero=zero):
                pltpu.make_async_copy(zero, dst, self.recv_sem).start()

    def start(self):
        for copy, to, source, dst in self.copies:
            pl.when(to)(copy.start)

    def recv(self):
        all_rows = self.dummy.at[0 : self.rows]
        pltpu.make_async_copy(all_rows, all_rows, self.recv_sem).wait()

    def sent(self):
        for copy, to, source, dst in self.copies:
            pl.when(to)(copy.wait_send)


def pick(d):
    return {-1: 0, 1: 1}[d]


def cut_strips(own, strips):
    f, p, r, _ = own.shape
    hy = strips.shape[3]
    for i in range(p):
        strips[0, :, i] = own[:, i, 0:hy, :]
        strips[1, :, i] = own[:, i, r - hy : r, :]


def add_xy(comm, own, strips, bufs, dz=0, deltas=XY):
    rx, ry, rc = bufs
    p, hx = own.shape[1], rx.shape[2]
    for dx, dy in deltas:
        xs = slice(0, hx) if dx < 0 else slice(p - hx, p)
        if dy == 0:
            src, dst = own.at[:, xs], rx.at[pick(-dx)]
        elif dx == 0:
            src, dst = strips.at[pick(dy)], ry.at[pick(-dy)]
        else:
            src, dst = strips.at[pick(dy), :, xs], rc.at[pick(-dx), pick(-dy)]
        comm.add((dx, dy, dz), src, dst)


def frame_halo(bufs, p, r, out):
    rx, ry, rc = bufs
    hx, hy = rx.shape[2], ry.shape[3]
    for sx, xs in ((0, slice(HALO - hx, HALO)), (1, slice(HALO + p, HALO + p + hx))):
        out[:, xs, HALO : HALO + r, :] = rx[sx]
        for sy, ys in ((0, slice(HALO - hy, HALO)), (1, slice(HALO + r, HALO + r + hy))):
            out[:, xs, ys, :] = rc[sx, sy]
    for sy, ys in ((0, slice(HALO - hy, HALO)), (1, slice(HALO + r, HALO + r + hy))):
        out[:, HALO : HALO + p, ys, :] = ry[sy]


def swap_blocks(regs, width, shift=0):
    n = len(regs)
    lane = lanes(regs[0].shape)
    into, outof = ((lane + shift) & 127) // width, lane // width
    bits = [1 << k for k in range(n.bit_length() - 1)]
    for bit in bits:
        mask = (into & bit) != 0
        regs = [jnp.where(mask, regs[(i + bit) % n], regs[i]) for i in range(n)]
    regs = [roll(regs[i], width * i + shift, 1) for i in range(n)]
    regs = [regs[-i % n] for i in range(n)]
    for bit in bits:
        mask = (outof & bit) != 0
        regs = [jnp.where(mask, regs[(i - bit) % n], regs[i]) for i in range(n)]
    return regs


def gather(x, index):
    return jnp.take_along_axis(x, index, axis=1, mode="promise_in_bounds")


def plan_block(v, place, weight):
    lane = lanes((8, 128))
    part = (lane >> 3) & 1
    ox, oy, oz = v & 7, (v >> 3) & 7, (v >> 6) & 7
    fx = ((v >> 9) & 7).astype(jnp.float32) * 0.125
    fy = ((v >> 12) & 7).astype(jnp.float32) * 0.125
    fz = ((v >> 15) & 7).astype(jnp.float32) * 0.125
    spot = (lane & 7) + oz + part
    place[0] = ((lane >> 4) + ox) * 8 + (spot & 7)
    place[1] = spot
    wz = jnp.where(part == 0, 1.0 - fz, fz)
    for dy in range(9):
        weight[dy] = jnp.where(oy == dy, 1.0 - fy, jnp.where(oy == dy - 1, fy, 0.0))
    weight[9] = (1.0 - fx) * wz
    weight[10] = fx * wz


def advect_block(place, weight, steps, load):
    near = place[1] < 8
    result = None
    for cx in range(2):
        index = place[0] + 8 * cx
        total = None
        for dy in steps:
            value = weight[dy] * jnp.where(near, gather(load(0, dy), index), gather(load(1, dy), index))
            total = value if total is None else total + value
        total = weight[9 + cx] * total
        result = total if result is None else result + total
    return result


def kernel(sizes, vel_hbm, den_hbm, off_hbm, eig_hbm, new_vel, new_den, press, off, eig, fetch_sem, fields, stripA, rxA, ryA, rcA, mixed,
           edge, gotP, src, code, place, weight, resT, u, extU, packU, wide, s0, q0, r0,
           tmp0, own1, strip1, rx1, ry1, rc1, rz1, ext1, wide1, q1, r1, tmp1, own2, got2, ext2, sum1, fine,
           sends, recvs, z32, z16, z8, z4, z2, dummy, *bufB):
    me = tuple(lax.axis_index(a) for a in ("gx", "gy", "gz"))
    p, r = fields.shape[1], fields.shape[2]
    p1, r1n = p // 2, r // 2
    p2, r2n = p1 // 2, r1n // 2
    pairs = [(vel_hbm, fields.at[0:3]), (den_hbm, fields.at[3]), (off_hbm, off), (eig_hbm, eig)]
    fetch = [pltpu.make_async_copy(a, b, fetch_sem.at[i]) for i, (a, b) in enumerate(pairs)]
    for copy in fetch:
        copy.start()
    barrier = pltpu.get_barrier_semaphore()
    peers = [(dx, dy, dz) for dz in (-1, 0, 1) for dx in (-1, 0, 1) for dy in (-1, 0, 1) if (dx, dy, dz) != (0, 0, 0)]
    count = jnp.int32(0)
    for delta in peers:
        ok = inside(sizes, me, delta)

        @pl.when(ok)
        def _():
            pl.semaphore_signal(barrier, inc=1, device_id=tuple(i + d for i, d in zip(me, delta)), device_id_type=MESH)

        count = count + jnp.where(ok, 1, 0)

    for zero in (z32, z16, z8, z4, z2):
        zero[...] = jnp.zeros(zero.shape, jnp.float32)
    made = []
    zeros = [z32, z16, z8, z4, z2]

    def comm(at):
        sems = [sends.at[i] for i in range(at, sends.shape[0])]
        made.append(Comm(sizes, me, sems, recvs.at[len(made)], zeros, dummy))
        return made[-1]

    commA = [comm(8 * c) for c in range(4)]
    for c in range(4):
        add_xy(commA[c], fields.at[c : c + 1], stripA.at[:, c : c + 1], (rxA.at[:, c : c + 1], ryA.at[:, c : c + 1], rcA.at[:, :, c : c + 1]))
    zA = [comm(32) for c in range(4)]
    for c in range(4):
        zA[c].add((0, 0, -1), edge.at[c], gotP.at[1, c])
        zA[c].add((0, 0, 1), edge.at[c], gotP.at[0, c])
    fieldB = [bufB[8 * c : 8 * c + 8] for c in range(3)]
    commB = [comm(0) for c in range(3)]
    for c, (strip, rx, ry, rc, edgeB, estrB, ezB, ezyB) in enumerate(fieldB):
        add_xy(commB[c], u.at[c : c + 1], strip, (rx, ry, rc))
        for dz in (-1, 1):
            for dx in (-1, 1, 0):
                for dy in (-1, 1):
                    commB[c].add((dx, dy, dz), estrB.at[pick(dy)], ezyB.at[pick(-dz), 1 - dx, pick(-dy)])
                commB[c].add((dx, 0, dz), edgeB, ezB.at[pick(-dz), 1 - dx])
    commC = comm(0)
    commD = comm(0)
    for dz in (-1, 1, 0):
        add_xy(commC, own1, strip1, (rx1.at[1 - dz], ry1.at[1 - dz], rc1.at[1 - dz]), dz, XY[4:] if dz else XY)
        for dx, dy in XY[4:] if dz else XY:
            commD.add((dx, dy, dz), own2, got2.at[1 - dz, 1 - dx, 1 - dy])
        if dz:
            commC.add((0, 0, dz), own1, rz1.at[pick(-dz)])
            commD.add((0, 0, dz), own2, got2.at[1 - dz, 1, 1])
    for each in made[:8]:
        each.missing()
    for z in (0, 2):
        rc1[z] = jnp.zeros(rc1.shape[1:], jnp.float32)
        for x in (0, 2):
            for y in (0, 2):
                got2[z, x, y] = jnp.zeros(got2.shape[3:], jnp.float32)
    ext2[...] = jnp.zeros(ext2.shape, jnp.float32)
    sum1[...] = jnp.zeros(sum1.shape, jnp.float32)
    for copy in fetch[:2]:
        copy.wait()
    cut_strips(fields, stripA)
    pl.semaphore_wait(barrier, count)
    for each in commA:
        each.start()
    for each in made[8:]:
        each.missing()

    even = ((lanes((8, 128)) >> 3) & 1) == 0

    def positions():
        for copy in fetch[2:]:
            copy.wait()
        whole = (off[0] + 4) + 8 * (off[1] + 4) + 64 * (off[2] + 4)
        code[...] = whole + 512 * eig[0] + 4096 * eig[1] + 32768 * eig[2]
        for t in range(r // 8):
            for q, v in enumerate(swap_blocks([code[x, 8 * t : 8 * t + 8] for x in range(p)], 16)):
                code[q, 8 * t : 8 * t + 8] = v
        for t in range(r // 8):

            def plan(q, carry):
                v = code[q, 8 * t : 8 * t + 8]
                plan_block(jnp.where(even, v, roll(v, 8, 1)), place.at[t, 2 * q], weight.at[t, 2 * q])
                plan_block(jnp.where(even, roll(v, -8, 1), v), place.at[t, 2 * q + 1], weight.at[t, 2 * q + 1])
                return carry

            lax.fori_loop(0, 8, plan, 0)

    positions()
    rows = r + 8
    blocks = 128 // 8
    half = r // 8
    lane16 = lanes((r, 128))
    lane = lanes((rows, 128))

    def advect(c, t, b):
        totals = advect_block(place.at[t, b], weight.at[t, b], range(9), lambda far, dy: src[c, b + far, 8 * t + 4 + dy : 8 * t + 12 + dy, :])
        resT[c, t, b] = totals

    def put(c, b, start, size, v):
        if b == 0:
            edge[c, start : start + size] = v
        else:
            src[c, b, start : start + size] = v

    low = (lanes((r + 16, 128)) & 7) < 4
    for c in range(4):
        commA[c].recv()
        for t in range(half):
            ys = slice(8 * t, 8 * t + 8)
            planes = [rxA[0, c, x, ys] for x in range(HALO)] + [fields[c, x, ys] for x in range(p)] + [rxA[1, c, x, ys] for x in range(HALO)]
            for b, v in enumerate(swap_blocks(planes, 8, 4)):
                put(c, b, 8 + 8 * t, 8, v)
        for side, at in ((1, 0), (0, 4)):
            for x in range(HALO):
                mixed[c, x, at : at + 4] = rcA[0, side, c, x]
                mixed[c, HALO + p + x, at : at + 4] = rcA[1, side, c, x]
            for x in range(p):
                mixed[c, HALO + x, at : at + 4] = ryA[side, c, x]
        for b, v in enumerate(swap_blocks([mixed[c, x] for x in range(p + 8)], 8, 4)):
            put(c, b, 4, 4, v[4:8])
            put(c, b, r + 8, 4, v[0:4])
        if c:
            zA[c - 1].sent()
        zA[c].start()
        for b in range(1, blocks - 1):
            for t in range(half):
                advect(c, t, b)
        zA[c].recv()
        src[c, 0] = jnp.where(low, gotP[0, c], edge[c])
        src[c, blocks] = jnp.where(low, edge[c], gotP[1, c])
        for b in (0, blocks - 1):
            for t in range(half):
                advect(c, t, b)
        for t in range(half):
            pairs = []
            for q in range(blocks // 2):
                one, two = resT[c, t, 2 * q], resT[c, t, 2 * q + 1]
                move = jnp.where(even, two, one)
                pairs.append(jnp.where(even, one, two) + jnp.where(even, roll(move, -8, 1), roll(move, 8, 1)))
            if c < 3:
                fieldB[c][4][8 * t : 8 * t + 8] = jnp.where(even, pairs[0], pairs[-1])
            for x, v in enumerate(swap_blocks(pairs, 16)):
                u[c, x, 8 * t : 8 * t + 8] = v
        if c == 3:
            new_den[...] = u[3]
            break
        strip, rx, ry, rc, edgeB, estrB, ezB, ezyB = fieldB[c]
        cut_strips(u.at[c : c + 1], strip)
        hy = estrB.shape[1]
        estrB[0] = edgeB[0:hy]
        estrB[1] = edgeB[r - hy : r]
        for each in commB[c - 1 : c] if c else commA:
            each.sent()
        commB[c].start()

    extU[:, HALO : HALO + p, HALO : HALO + r, :] = u[0:3]
    zA[3].sent()
    commB[2].sent()

    def edges(lo, hi):
        return jnp.where((lanes(lo.shape) & 15) < 8, hi, roll(lo, -16, 1))

    def yz_mask(nrows, first_row, block_rows, cells):
        row = lax.broadcasted_iota(jnp.int32, (nrows, 256), 0) - first_row + me[1] * block_rows
        spot = lanes((nrows, 256))
        z = jnp.where(spot < 192, spot, spot - 256) + me[2] * cells
        return (row >= 0) & (row < sizes[1] * block_rows) & (z >= 0) & (z < sizes[2] * cells)

    def x_ok(x, first, block):
        g = x - first + me[0] * block
        return (g >= 0) & (g < sizes[0] * block)

    mask0 = yz_mask(rows, HALO, r, 128)

    def around(ref, x, step):
        v = ref[x]
        total = ref[x + 1] + ref[x - 1]
        total = total + roll(v, -1, 0) + roll(v, 1, 0)
        total = total + roll(v, -step, 1) + roll(v, step, 1)
        return 6.0 * v - total

    def second(ref, x, scale, step):
        v = ref[x]
        first = (RELAX * scale) * v
        return first + RELAX * (scale * v - (RELAX * scale) * around(ref, x, step))

    for c, (strip, rx, ry, rc, edgeB, estrB, ezB, ezyB) in enumerate(fieldB):
        commB[c].recv()
        frame_halo((rx, ry, rc), p, r, extU.at[c : c + 1])
        hy = estrB.shape[1]
        for i in range(3):
            packU[c, i, HALO : HALO + r] = edges(ezB[0, i], ezB[1, i])
            for sy, ys in ((0, slice(HALO - hy, HALO)), (1, slice(HALO + r, HALO + r + hy))):
                packU[c, i, ys] = edges(ezyB[0, i, sy], ezyB[1, i, sy])
        for x in range(HALO - 3, HALO + p + 3):
            wide[c, x, :, 0:128] = extU[c, x]
            i = 0 if x < HALO else 1 if x < HALO + p else 2
            wide[c, x, :, 128:256] = roll(packU[c, i], -16 * ((x - HALO) % p), 1)
        for x in range(HALO - 2, HALO + p + 2):
            if c == 0:
                s0[x] = wide[0, x + 1] - wide[0, x - 1]
            elif c == 1:
                v = wide[1, x]
                s0[x] = s0[x] + (roll(v, -1, 0) - roll(v, 1, 0))
            else:
                v = wide[2, x]
                part = s0[x] + (roll(v, -1, 1) - roll(v, 1, 1))
                s0[x] = jnp.where(mask0 & x_ok(x, HALO, p), -0.5 * part, 0.0)

    for x in range(HALO - 1, HALO + p + 1):
        q0[x] = jnp.where(mask0 & x_ok(x, HALO, p), second(s0, x, 1.0, 1), 0.0)
    for x in range(HALO, HALO + p):
        r0[x] = (s0[x] - around(q0, x, 1))[:, 0:128]
    lane8 = lanes((r // 2, 128))
    for x in range(p // 2):
        tmp0[...] = r0[HALO + 2 * x] + r0[HALO + 2 * x + 1]
        v = tmp0[pl.ds(HALO, r // 2, stride=2), :] + tmp0[pl.ds(HALO + 1, r // 2, stride=2), :]
        v = v + jnp.where((lane8 & 1) == 0, roll(v, -1, 1), roll(v, 1, 1))
        own1[0, x] = 0.125 * v

    cut_strips(own1, strip1)
    commC.start()
    commC.sent()
    commC.recv()
    rows1 = r1n + 8
    for dz in range(3):
        ext1[dz, :, HALO : HALO + p1, HALO : HALO + r1n, :] = own1[...] if dz == 1 else rz1[dz // 2]
        frame_halo((rx1.at[dz], ry1.at[dz], rc1.at[dz]), p1, r1n, ext1.at[dz])
    lane1 = lanes((rows1, 128))
    for x in range(HALO - 2, HALO + p1 + 2):
        wide1[x, :, 0:128] = ext1[1, 0, x]
        wide1[x, :, 128:256] = jnp.where(lane1 < 64, ext1[2, 0, x], ext1[0, 0, x])
    mask1 = yz_mask(rows1, HALO, r1n, 128)
    for x in range(HALO - 1, HALO + p1 + 1):
        q1[x] = jnp.where(mask1 & x_ok(x, HALO, p1), second(wide1, x, 4.0, 2), 0.0)
    for x in range(HALO, HALO + p1):
        r1[x] = (wide1[x] - 0.25 * around(q1, x, 2))[:, 0:128]
    lane4 = lanes((r2n, 128))
    for x in range(p2):
        tmp1[...] = r1[HALO + 2 * x] + r1[HALO + 2 * x + 1]
        v = tmp1[pl.ds(HALO, r2n, stride=2), :] + tmp1[pl.ds(HALO + 1, r2n, stride=2), :]
        v = v + jnp.where((lane4 & 3) < 2, roll(v, -2, 1), roll(v, 2, 1))
        own2[x] = 0.125 * v

    commD.start()
    got2[1, 1, 1] = own2[...]
    commD.sent()
    commD.recv()
    for z in range(3):
        for a in range(3):
            for b in range(3):
                ext2[z, p2 * a : p2 * a + p2, r2n * b : r2n * b + r2n, :] = got2[z, a, b]
    lane2 = lanes((16, 128))
    mask2 = yz_mask(16, r2n, r2n, 128)
    planes2 = {}
    for x in range(p2 - 2, 2 * p2 + 2):
        planes2[x] = jnp.concatenate([ext2[1, x], jnp.where(lane2 < 64, ext2[2, x], ext2[0, x])], axis=1)
    for x in range(p2 - 1, 2 * p2 + 1):
        v = jnp.where(mask2 & x_ok(x, p2, p2), second(planes2, x, 16.0, 4), 0.0)
        first_row = r2n - 1
        take = r2n + 2
        base = HALO - 2
        for side in range(2):
            part = v[first_row : first_row + take, 128 * side : 128 * side + 128]
            sum1[x, side, pl.ds(base, take, stride=2), :] = part
            sum1[x, side, pl.ds(base + 1, take, stride=2), :] = part
    for x1 in range(HALO - 1, HALO + p1 + 1):
        x2 = (x1 - HALO) // 2 + p2
        for side in range(2):
            v = q1[x1, :, 128 * side : 128 * side + 128] + sum1[x2, side]
            part = v[HALO - 2 : HALO - 2 + r1n + 4]
            fine[x1, side, pl.ds(0, r1n + 4, stride=2), :] = part
            fine[x1, side, pl.ds(1, r1n + 4, stride=2), :] = part
    for x in range(HALO - 1, HALO + p + 1):
        x1 = (x - HALO) // 2 + HALO
        coarse = jnp.concatenate([fine[x1, 0], fine[x1, 1]], axis=1)
        s0[x] = jnp.where(mask0 & x_ok(x, HALO, p), q0[x] + coarse, 0.0)
    for x in range(p):
        v = s0[x + HALO]
        cut = lambda t: t[HALO : HALO + r, 0:128]
        press[x] = cut(v)
        new_vel[0, x] = u[0, x] - 0.5 * cut(s0[x + HALO + 1] - s0[x + HALO - 1])
        new_vel[1, x] = u[1, x] - 0.5 * cut(roll(v, -1, 0) - roll(v, 1, 0))
        new_vel[2, x] = u[2, x] - 0.5 * cut(roll(v, -1, 1) - roll(v, 1, 1))


def write_kernel(*refs):
    n = len(refs) // 2
    copies = [pltpu.make_async_copy(refs[i], refs[n + i], refs[-1].at[i]) for i in range(n)]
    for copy in copies:
        copy.start()
    for copy in copies:
        copy.wait()


def write_out(results):
    return pl.pallas_call(
        write_kernel,
        out_shape=tuple(jax.ShapeDtypeStruct(a.shape, a.dtype) for a in results),
        in_specs=[pl.BlockSpec(memory_space=pltpu.VMEM)] * len(results),
        out_specs=(pl.BlockSpec(memory_space=pltpu.HBM),) * len(results),
        scratch_shapes=[pltpu.SemaphoreType.DMA((len(results),))],
        compiler_params=pltpu.CompilerParams(vmem_limit_bytes=1 << 20),
    )(*results)


def step(sizes, velocity, density, offsets, eighths):
    p, r, _ = density.shape
    f32 = jnp.float32

    def vm(*shape):
        return pltpu.VMEM(shape, f32)

    def xy(f, p, r, hx, hy):
        return [vm(2, f, p, hy, 128), vm(2, f, hx, r, 128), vm(2, f, p, hy, 128), vm(2, 2, f, hx, hy, 128)]

    assert p == 8 and r % 8 == 0
    p1, r1, p2, r2 = p // 2, r // 2, p // 4, r // 4
    rows, rows1 = r + 8, r1 + 8
    dma = lambda *n: pltpu.SemaphoreType.DMA(n)
    half = r // 8
    scratch = (
        [pltpu.VMEM(offsets.shape, jnp.int32), pltpu.VMEM(eighths.shape, jnp.int32), dma(4), vm(4, p, r, 128)] + xy(4, p, r, 4, 4)
        + [vm(4, p + 8, 8, 128), vm(4, r + 16, 128), vm(2, 4, r + 16, 128), vm(4, 17, r + 16, 128),
           pltpu.VMEM((p, r, 128), jnp.int32), pltpu.VMEM((half, 16, 2, 8, 128), jnp.int32), vm(half, 16, 11, 8, 128),
           vm(4, half, 16, 8, 128), vm(4, p, r, 128)]
        + [vm(3, p + 8, rows, 128), vm(3, 3, rows, 128), vm(3, p + 8, rows, 256),
           vm(p + 8, rows, 256), vm(p + 8, rows, 256), vm(p + 8, rows, 128), vm(rows, 128), vm(1, p1, r1, 128)]
        + [vm(2, 1, p1, 2, 128), vm(3, 2, 1, 2, r1, 128), vm(3, 2, 1, p1, 2, 128), vm(3, 2, 2, 1, 2, 2, 128), vm(2, 1, p1, r1, 128)]
        + [vm(3, 1, p1 + 8, rows1, 128), vm(p1 + 8, rows1, 256), vm(p1 + 8, rows1, 256),
           vm(p1 + 8, rows1, 128), vm(rows1, 128), vm(p2, r2, 128), vm(3, 3, 3, p2, r2, 128), vm(3, 3 * p2, 16, 128),
           vm(3 * p2, 2, rows1, 128), vm(p1 + 8, 2, rows, 128)]
        + [dma(34), dma(13), vm(1, 1, r + 16, 128), vm(1, 4, r, 128), vm(1, 4, 8, 128), vm(1, 8, 4, 128), vm(1, 8, 2, 128), vm(512, 128)]
    )
    for hx, hy in ((3, 2), (2, 4), (2, 2)):
        scratch += xy(1, p, r, hx, hy) + [vm(r, 128), vm(2, hy, 128), vm(2, 3, r, 128), vm(2, 3, 2, hy, 128)]
    vmem = pl.BlockSpec(memory_space=pltpu.VMEM)
    results = pl.pallas_call(
        functools.partial(kernel, sizes),
        out_shape=(
            jax.ShapeDtypeStruct(velocity.shape, f32),
            jax.ShapeDtypeStruct(density.shape, f32),
            jax.ShapeDtypeStruct(density.shape, f32),
        ),
        in_specs=[pl.BlockSpec(memory_space=pltpu.HBM)] * 4,
        out_specs=(vmem,) * 3,
        scratch_shapes=scratch,
        compiler_params=pltpu.CompilerParams(
            collective_id=0, has_side_effects=True, vmem_limit_bytes=32 * 1024 * 1024
        ),
    )(*[pltpu.with_memory_space_constraint(a, pltpu.HBM) for a in (velocity, density, offsets, eighths)])
    return write_out(results)


def solution(mesh):
    sizes = tuple(mesh.shape[a] for a in ("gx", "gy", "gz"))
    block = P("gx", "gy", "gz")
    stacked = P(None, "gx", "gy", "gz")
    return jax.shard_map(
        functools.partial(step, sizes),
        mesh=mesh,
        in_specs=(stacked, block, stacked, stacked),
        out_specs=(stacked, block, block),
        check_vma=False,
    )
```

```python
import functools
import math

import jax
import jax.numpy as jnp
from jax import lax
from jax.experimental import pallas as pl
from jax.experimental.pallas import tpu as pltpu
from jax.sharding import PartitionSpec as P

MESH = pl.DeviceIdType.MESH
RELAX = (6.0 / 7.0) / 6.0
HALO = 4
XY = [(-1, -1), (-1, 1), (1, -1), (1, 1), (-1, 0), (1, 0), (0, -1), (0, 1)]


def lanes(shape):
    return lax.broadcasted_iota(jnp.int32, shape, len(shape) - 1)


def roll(x, shift, axis):
    shift = shift % x.shape[axis]
    return x if shift == 0 else pltpu.roll(x, shift, axis)


def inside(sizes, me, delta):
    ok = None
    for n, i, d in zip(sizes, me, delta):
        if d:
            one = (i + d >= 0) & (i + d < n)
            ok = one if ok is None else ok & one
    return ok


class Comm:
    def __init__(self, sizes, me, sends, recv, zeros, dummy):
        self.sizes, self.me, self.sends, self.recv_sem = sizes, me, sends, recv
        self.zeros, self.dummy = zeros, dummy
        self.copies, self.rows = [], 0

    def add(self, delta, src, dst):
        device = tuple(i + d for i, d in zip(self.me, delta))
        copy = pltpu.make_async_remote_copy(
            src_ref=src, dst_ref=dst, send_sem=self.sends[len(self.copies)], recv_sem=self.recv_sem,
            device_id=device, device_id_type=MESH,
        )
        to = inside(self.sizes, self.me, delta)
        source = inside(self.sizes, self.me, tuple(-d for d in delta))
        self.copies.append((copy, to, source, dst))
        self.rows += math.prod(dst.shape) // 128

    def missing(self):
        for copy, to, source, dst in self.copies:
            zero = next(z for z in self.zeros if z.shape[2] == dst.shape[-2])
            n = dst.shape[-3] if len(dst.shape) > 2 else 1
            zero = zero.at[:, 0:n] if len(dst.shape) == 4 else zero.at[0, 0:n] if len(dst.shape) == 3 else zero.at[0, 0]

            @pl.when(jnp.logical_not(source))
            def _(dst=dst, zero=zero):
                pltpu.make_async_copy(zero, dst, self.recv_sem).start()

    def start(self):
        for copy, to, source, dst in self.copies:
            pl.when(to)(copy.start)

    def recv(self):
        all_rows = self.dummy.at[0 : self.rows]
        pltpu.make_async_copy(all_rows, all_rows, self.recv_sem).wait()

    def sent(self):
        for copy, to, source, dst in self.copies:
            pl.when(to)(copy.wait_send)


def pick(d):
    return {-1: 0, 1: 1}[d]


def cut_strips(own, strips):
    f, p, r, _ = own.shape
    hy = strips.shape[3]
    for i in range(p):
        strips[0, :, i] = own[:, i, 0:hy, :]
        strips[1, :, i] = own[:, i, r - hy : r, :]


def add_xy(comm, own, strips, bufs, dz=0, deltas=XY):
    rx, ry, rc = bufs
    p, hx = own.shape[1], rx.shape[2]
    for dx, dy in deltas:
        xs = slice(0, hx) if dx < 0 else slice(p - hx, p)
        if dy == 0:
            src, dst = own.at[:, xs], rx.at[pick(-dx)]
        elif dx == 0:
            src, dst = strips.at[pick(dy)], ry.at[pick(-dy)]
        else:
            src, dst = strips.at[pick(dy), :, xs], rc.at[pick(-dx), pick(-dy)]
        comm.add((dx, dy, dz), src, dst)


def frame_halo(bufs, p, r, out):
    rx, ry, rc = bufs
    hx, hy = rx.shape[2], ry.shape[3]
    for sx, xs in ((0, slice(HALO - hx, HALO)), (1, slice(HALO + p, HALO + p + hx))):
        out[:, xs, HALO : HALO + r, :] = rx[sx]
        for sy, ys in ((0, slice(HALO - hy, HALO)), (1, slice(HALO + r, HALO + r + hy))):
            out[:, xs, ys, :] = rc[sx, sy]
    for sy, ys in ((0, slice(HALO - hy, HALO)), (1, slice(HALO + r, HALO + r + hy))):
        out[:, HALO : HALO + p, ys, :] = ry[sy]


def swap_blocks(regs, width, shift=0):
    n = len(regs)
    lane = lanes(regs[0].shape)
    into, outof = ((lane + shift) & 127) // width, lane // width
    bits = [1 << k for k in range(n.bit_length() - 1)]
    for bit in bits:
        mask = (into & bit) != 0
        regs = [jnp.where(mask, regs[(i + bit) % n], regs[i]) for i in range(n)]
    regs = [roll(regs[i], width * i + shift, 1) for i in range(n)]
    regs = [regs[-i % n] for i in range(n)]
    for bit in bits:
        mask = (outof & bit) != 0
        regs = [jnp.where(mask, regs[(i - bit) % n], regs[i]) for i in range(n)]
    return regs


def gather(x, index):
    return jnp.take_along_axis(x, index, axis=1, mode="promise_in_bounds")


def plan_block(v, place, weight):
    lane = lanes((8, 128))
    part = (lane >> 3) & 1
    ox, oy, oz = v & 7, (v >> 3) & 7, (v >> 6) & 7
    fx = ((v >> 9) & 7).astype(jnp.float32) * 0.125
    fy = ((v >> 12) & 7).astype(jnp.float32) * 0.125
    fz = ((v >> 15) & 7).astype(jnp.float32) * 0.125
    spot = (lane & 7) + oz + part
    place[0] = ((lane >> 4) + ox) * 8 + (spot & 7)
    place[1] = spot
    wz = jnp.where(part == 0, 1.0 - fz, fz)
    for dy in range(9):
        weight[dy] = jnp.where(oy == dy, 1.0 - fy, jnp.where(oy == dy - 1, fy, 0.0))
    weight[9] = (1.0 - fx) * wz
    weight[10] = fx * wz


def advect_block(place, weight, steps, load):
    near = place[1] < 8
    result = None
    for cx in range(2):
        index = place[0] + 8 * cx
        total = None
        for dy in steps:
            value = weight[dy] * jnp.where(near, gather(load(0, dy), index), gather(load(1, dy), index))
            total = value if total is None else total + value
        total = weight[9 + cx] * total
        result = total if result is None else result + total
    return result


def kernel(sizes, vel_hbm, den_hbm, off_hbm, eig_hbm, new_vel, new_den, press, off, eig, fetch_sem, fields, stripA, rxA, ryA, rcA, mixed,
           edge, gotP, src, code, place, weight, resT, u, extU, packU, wide, s0, q0, r0,
           tmp0, own1, strip1, rx1, ry1, rc1, rz1, ext1, wide1, q1, r1, tmp1, own2, got2, ext2, sum1, fine,
           sends, recvs, z32, z16, z8, z4, z2, dummy, *bufB):
    me = tuple(lax.axis_index(a) for a in ("gx", "gy", "gz"))
    p, r = fields.shape[1], fields.shape[2]
    p1, r1n = p // 2, r // 2
    p2, r2n = p1 // 2, r1n // 2
    pairs = [(vel_hbm, fields.at[0:3]), (den_hbm, fields.at[3]), (off_hbm, off), (eig_hbm, eig)]
    fetch = [pltpu.make_async_copy(a, b, fetch_sem.at[i]) for i, (a, b) in enumerate(pairs)]
    for copy in fetch:
        copy.start()
    barrier = pltpu.get_barrier_semaphore()
    peers = [(dx, dy, dz) for dz in (-1, 0, 1) for dx in (-1, 0, 1) for dy in (-1, 0, 1) if (dx, dy, dz) != (0, 0, 0)]
    count = jnp.int32(0)
    for delta in peers:
        ok = inside(sizes, me, delta)

        @pl.when(ok)
        def _():
            pl.semaphore_signal(barrier, inc=1, device_id=tuple(i + d for i, d in zip(me, delta)), device_id_type=MESH)

        count = count + jnp.where(ok, 1, 0)

    for zero in (z32, z16, z8, z4, z2):
        zero[...] = jnp.zeros(zero.shape, jnp.float32)
    made = []
    zeros = [z32, z16, z8, z4, z2]

    def comm(at):
        sems = [sends.at[i] for i in range(at, sends.shape[0])]
        made.append(Comm(sizes, me, sems, recvs.at[len(made)], zeros, dummy))
        return made[-1]

    commA = [comm(8 * c) for c in range(4)]
    for c in range(4):
        add_xy(commA[c], fields.at[c : c + 1], stripA.at[:, c : c + 1], (rxA.at[:, c : c + 1], ryA.at[:, c : c + 1], rcA.at[:, :, c : c + 1]))
    zA = [comm(32) for c in range(4)]
    for c in range(4):
        zA[c].add((0, 0, -1), edge.at[c], gotP.at[1, c])
        zA[c].add((0, 0, 1), edge.at[c], gotP.at[0, c])
    fieldB = [bufB[8 * c : 8 * c + 8] for c in range(3)]
    commB = [comm(0) for c in range(3)]
    for c, (strip, rx, ry, rc, edgeB, estrB, ezB, ezyB) in enumerate(fieldB):
        for dx, dy in XY[:4]:
            for dz in (-1, 1):
                commB[c].add((dx, dy, dz), estrB.at[pick(dy)], ezyB.at[pick(-dz), 1 - dx, pick(-dy)])
        add_xy(commB[c], u.at[c : c + 1], strip, (rx, ry, rc))
        for dz in (-1, 1):
            for dx in (-1, 1):
                commB[c].add((dx, 0, dz), edgeB, ezB.at[pick(-dz), 1 - dx])
            for dy in (-1, 1):
                commB[c].add((0, dy, dz), estrB.at[pick(dy)], ezyB.at[pick(-dz), 1, pick(-dy)])
            commB[c].add((0, 0, dz), edgeB, ezB.at[pick(-dz), 1])
    commC = comm(0)
    commD = comm(0)
    for dz in (0, -1, 1):
        add_xy(commC, own1, strip1, (rx1.at[1 - dz], ry1.at[1 - dz], rc1.at[1 - dz]), dz, XY[4:] if dz else XY)
        for dx, dy in XY[4:] if dz else XY:
            commD.add((dx, dy, dz), own2, got2.at[1 - dz, 1 - dx, 1 - dy])
        if dz:
            commC.add((0, 0, dz), own1, rz1.at[pick(-dz)])
            commD.add((0, 0, dz), own2, got2.at[1 - dz, 1, 1])
    for each in made[:8]:
        each.missing()
    for z in (0, 2):
        rc1[z] = jnp.zeros(rc1.shape[1:], jnp.float32)
        for x in (0, 2):
            for y in (0, 2):
                got2[z, x, y] = jnp.zeros(got2.shape[3:], jnp.float32)
    ext2[...] = jnp.zeros(ext2.shape, jnp.float32)
    sum1[...] = jnp.zeros(sum1.shape, jnp.float32)
    for copy in fetch[:2]:
        copy.wait()
    cut_strips(fields, stripA)
    pl.semaphore_wait(barrier, count)
    for each in commA:
        each.start()
    for each in made[8:]:
        each.missing()

    even = ((lanes((8, 128)) >> 3) & 1) == 0

    def positions():
        for copy in fetch[2:]:
            copy.wait()
        whole = (off[0] + 4) + 8 * (off[1] + 4) + 64 * (off[2] + 4)
        code[...] = whole + 512 * eig[0] + 4096 * eig[1] + 32768 * eig[2]
        for t in range(r // 8):
            for q, v in enumerate(swap_blocks([code[x, 8 * t : 8 * t + 8] for x in range(p)], 16)):
                code[q, 8 * t : 8 * t + 8] = v
        for t in range(r // 8):

            def plan(q, carry):
                v = code[q, 8 * t : 8 * t + 8]
                plan_block(jnp.where(even, v, roll(v, 8, 1)), place.at[t, 2 * q], weight.at[t, 2 * q])
                plan_block(jnp.where(even, roll(v, -8, 1), v), place.at[t, 2 * q + 1], weight.at[t, 2 * q + 1])
                return carry

            lax.fori_loop(0, 8, plan, 0)

    positions()
    rows = r + 8
    blocks = 128 // 8
    half = r // 8
    lane16 = lanes((r, 128))
    lane = lanes((rows, 128))

    def advect(c, t, b):
        totals = advect_block(place.at[t, b], weight.at[t, b], range(9), lambda far, dy: src[c, b + far, 8 * t + 4 + dy : 8 * t + 12 + dy, :])
        resT[c, t, b] = totals

    def put(c, b, start, size, v):
        if b == 0:
            edge[c, start : start + size] = v
        else:
            src[c, b, start : start + size] = v

    low = (lanes((r + 16, 128)) & 7) < 4
    for c in range(4):
        commA[c].recv()
        for t in range(half):
            ys = slice(8 * t, 8 * t + 8)
            planes = [rxA[0, c, x, ys] for x in range(HALO)] + [fields[c, x, ys] for x in range(p)] + [rxA[1, c, x, ys] for x in range(HALO)]
            for b, v in enumerate(swap_blocks(planes, 8, 4)):
                put(c, b, 8 + 8 * t, 8, v)
        for side, at in ((1, 0), (0, 4)):
            for x in range(HALO):
                mixed[c, x, at : at + 4] = rcA[0, side, c, x]
                mixed[c, HALO + p + x, at : at + 4] = rcA[1, side, c, x]
            for x in range(p):
                mixed[c, HALO + x, at : at + 4] = ryA[side, c, x]
        for b, v in enumerate(swap_blocks([mixed[c, x] for x in range(p + 8)], 8, 4)):
            put(c, b, 4, 4, v[4:8])
            put(c, b, r + 8, 4, v[0:4])
        if c:
            zA[c - 1].sent()
        zA[c].start()
        for b in range(1, blocks - 1):
            for t in range(half):
                advect(c, t, b)
        zA[c].recv()
        src[c, 0] = jnp.where(low, gotP[0, c], edge[c])
        src[c, blocks] = jnp.where(low, edge[c], gotP[1, c])
        for b in (0, blocks - 1):
            for t in range(half):
                advect(c, t, b)
        for t in range(half):
            pairs = []
            for q in range(blocks // 2):
                one, two = resT[c, t, 2 * q], resT[c, t, 2 * q + 1]
                move = jnp.where(even, two, one)
                pairs.append(jnp.where(even, one, two) + jnp.where(even, roll(move, -8, 1), roll(move, 8, 1)))
            if c < 3:
                fieldB[c][4][8 * t : 8 * t + 8] = jnp.where(even, pairs[0], pairs[-1])
            for x, v in enumerate(swap_blocks(pairs, 16)):
                u[c, x, 8 * t : 8 * t + 8] = v
        if c == 3:
            new_den[...] = u[3]
            break
        strip, rx, ry, rc, edgeB, estrB, ezB, ezyB = fieldB[c]
        cut_strips(u.at[c : c + 1], strip)
        hy = estrB.shape[1]
        estrB[0] = edgeB[0:hy]
        estrB[1] = edgeB[r - hy : r]
        for each in commB[c - 1 : c] if c else commA:
            each.sent()
        commB[c].start()

    extU[:, HALO : HALO + p, HALO : HALO + r, :] = u[0:3]
    zA[3].sent()
    commB[2].sent()

    def edges(lo, hi):
        return jnp.where((lanes(lo.shape) & 15) < 8, hi, roll(lo, -16, 1))

    def yz_mask(nrows, first_row, block_rows, cells):
        row = lax.broadcasted_iota(jnp.int32, (nrows, 256), 0) - first_row + me[1] * block_rows
        spot = lanes((nrows, 256))
        z = jnp.where(spot < 192, spot, spot - 256) + me[2] * cells
        return (row >= 0) & (row < sizes[1] * block_rows) & (z >= 0) & (z < sizes[2] * cells)

    def x_ok(x, first, block):
        g = x - first + me[0] * block
        return (g >= 0) & (g < sizes[0] * block)

    mask0 = yz_mask(rows, HALO, r, 128)

    def around(ref, x, step):
        v = ref[x]
        total = ref[x + 1] + ref[x - 1]
        total = total + roll(v, -1, 0) + roll(v, 1, 0)
        total = total + roll(v, -step, 1) + roll(v, step, 1)
        return 6.0 * v - total

    def second(ref, x, scale, step):
        v = ref[x]
        first = (RELAX * scale) * v
        return first + RELAX * (scale * v - (RELAX * scale) * around(ref, x, step))

    for c, (strip, rx, ry, rc, edgeB, estrB, ezB, ezyB) in enumerate(fieldB):
        commB[c].recv()
        frame_halo((rx, ry, rc), p, r, extU.at[c : c + 1])
        hy = estrB.shape[1]
        for i in range(3):
            packU[c, i, HALO : HALO + r] = edges(ezB[0, i], ezB[1, i])
            for sy, ys in ((0, slice(HALO - hy, HALO)), (1, slice(HALO + r, HALO + r + hy))):
                packU[c, i, ys] = edges(ezyB[0, i, sy], ezyB[1, i, sy])
        for x in range(HALO - 3, HALO + p + 3):
            wide[c, x, :, 0:128] = extU[c, x]
            i = 0 if x < HALO else 1 if x < HALO + p else 2
            wide[c, x, :, 128:256] = roll(packU[c, i], -16 * ((x - HALO) % p), 1)
        for x in range(HALO - 2, HALO + p + 2):
            if c == 0:
                s0[x] = wide[0, x + 1] - wide[0, x - 1]
            elif c == 1:
                v = wide[1, x]
                s0[x] = s0[x] + (roll(v, -1, 0) - roll(v, 1, 0))
            else:
                v = wide[2, x]
                part = s0[x] + (roll(v, -1, 1) - roll(v, 1, 1))
                s0[x] = jnp.where(mask0 & x_ok(x, HALO, p), -0.5 * part, 0.0)

    for x in range(HALO - 1, HALO + p + 1):
        q0[x] = jnp.where(mask0 & x_ok(x, HALO, p), second(s0, x, 1.0, 1), 0.0)
    for x in range(HALO, HALO + p):
        r0[x] = (s0[x] - around(q0, x, 1))[:, 0:128]
    lane8 = lanes((r // 2, 128))
    for x in range(p // 2):
        tmp0[...] = r0[HALO + 2 * x] + r0[HALO + 2 * x + 1]
        v = tmp0[pl.ds(HALO, r // 2, stride=2), :] + tmp0[pl.ds(HALO + 1, r // 2, stride=2), :]
        v = v + jnp.where((lane8 & 1) == 0, roll(v, -1, 1), roll(v, 1, 1))
        own1[0, x] = 0.125 * v

    cut_strips(own1, strip1)
    commC.start()
    commC.sent()
    commC.recv()
    rows1 = r1n + 8
    for dz in range(3):
        ext1[dz, :, HALO : HALO + p1, HALO : HALO + r1n, :] = own1[...] if dz == 1 else rz1[dz // 2]
        frame_halo((rx1.at[dz], ry1.at[dz], rc1.at[dz]), p1, r1n, ext1.at[dz])
    lane1 = lanes((rows1, 128))
    for x in range(HALO - 2, HALO + p1 + 2):
        wide1[x, :, 0:128] = ext1[1, 0, x]
        wide1[x, :, 128:256] = jnp.where(lane1 < 64, ext1[2, 0, x], ext1[0, 0, x])
    mask1 = yz_mask(rows1, HALO, r1n, 128)
    for x in range(HALO - 1, HALO + p1 + 1):
        q1[x] = jnp.where(mask1 & x_ok(x, HALO, p1), second(wide1, x, 4.0, 2), 0.0)
    for x in range(HALO, HALO + p1):
        r1[x] = (wide1[x] - 0.25 * around(q1, x, 2))[:, 0:128]
    lane4 = lanes((r2n, 128))
    for x in range(p2):
        tmp1[...] = r1[HALO + 2 * x] + r1[HALO + 2 * x + 1]
        v = tmp1[pl.ds(HALO, r2n, stride=2), :] + tmp1[pl.ds(HALO + 1, r2n, stride=2), :]
        v = v + jnp.where((lane4 & 3) < 2, roll(v, -2, 1), roll(v, 2, 1))
        own2[x] = 0.125 * v

    commD.start()
    got2[1, 1, 1] = own2[...]
    commD.sent()
    commD.recv()
    for z in range(3):
        for a in range(3):
            for b in range(3):
                ext2[z, p2 * a : p2 * a + p2, r2n * b : r2n * b + r2n, :] = got2[z, a, b]
    lane2 = lanes((16, 128))
    mask2 = yz_mask(16, r2n, r2n, 128)
    planes2 = {}
    for x in range(p2 - 2, 2 * p2 + 2):
        planes2[x] = jnp.concatenate([ext2[1, x], jnp.where(lane2 < 64, ext2[2, x], ext2[0, x])], axis=1)
    for x in range(p2 - 1, 2 * p2 + 1):
        v = jnp.where(mask2 & x_ok(x, p2, p2), second(planes2, x, 16.0, 4), 0.0)
        first_row = r2n - 1
        take = r2n + 2
        base = HALO - 2
        for side in range(2):
            part = v[first_row : first_row + take, 128 * side : 128 * side + 128]
            sum1[x, side, pl.ds(base, take, stride=2), :] = part
            sum1[x, side, pl.ds(base + 1, take, stride=2), :] = part
    for x1 in range(HALO - 1, HALO + p1 + 1):
        x2 = (x1 - HALO) // 2 + p2
        for side in range(2):
            v = q1[x1, :, 128 * side : 128 * side + 128] + sum1[x2, side]
            part = v[HALO - 2 : HALO - 2 + r1n + 4]
            fine[x1, side, pl.ds(0, r1n + 4, stride=2), :] = part
            fine[x1, side, pl.ds(1, r1n + 4, stride=2), :] = part
    for x in range(HALO - 1, HALO + p + 1):
        x1 = (x - HALO) // 2 + HALO
        coarse = jnp.concatenate([fine[x1, 0], fine[x1, 1]], axis=1)
        s0[x] = jnp.where(mask0 & x_ok(x, HALO, p), q0[x] + coarse, 0.0)
    for x in range(p):
        v = s0[x + HALO]
        cut = lambda t: t[HALO : HALO + r, 0:128]
        press[x] = cut(v)
        new_vel[0, x] = u[0, x] - 0.5 * cut(s0[x + HALO + 1] - s0[x + HALO - 1])
        new_vel[1, x] = u[1, x] - 0.5 * cut(roll(v, -1, 0) - roll(v, 1, 0))
        new_vel[2, x] = u[2, x] - 0.5 * cut(roll(v, -1, 1) - roll(v, 1, 1))


def write_kernel(*refs):
    n = len(refs) // 2
    copies = [pltpu.make_async_copy(refs[i], refs[n + i], refs[-1].at[i]) for i in range(n)]
    for copy in copies:
        copy.start()
    for copy in copies:
        copy.wait()


def write_out(results):
    return pl.pallas_call(
        write_kernel,
        out_shape=tuple(jax.ShapeDtypeStruct(a.shape, a.dtype) for a in results),
        in_specs=[pl.BlockSpec(memory_space=pltpu.VMEM)] * len(results),
        out_specs=(pl.BlockSpec(memory_space=pltpu.HBM),) * len(results),
        scratch_shapes=[pltpu.SemaphoreType.DMA((len(results),))],
        compiler_params=pltpu.CompilerParams(vmem_limit_bytes=1 << 20),
    )(*results)


def step(sizes, velocity, density, offsets, eighths):
    p, r, _ = density.shape
    f32 = jnp.float32

    def vm(*shape):
        return pltpu.VMEM(shape, f32)

    def xy(f, p, r, hx, hy):
        return [vm(2, f, p, hy, 128), vm(2, f, hx, r, 128), vm(2, f, p, hy, 128), vm(2, 2, f, hx, hy, 128)]

    assert p == 8 and r % 8 == 0
    p1, r1, p2, r2 = p // 2, r // 2, p // 4, r // 4
    rows, rows1 = r + 8, r1 + 8
    dma = lambda *n: pltpu.SemaphoreType.DMA(n)
    half = r // 8
    scratch = (
        [pltpu.VMEM(offsets.shape, jnp.int32), pltpu.VMEM(eighths.shape, jnp.int32), dma(4), vm(4, p, r, 128)] + xy(4, p, r, 4, 4)
        + [vm(4, p + 8, 8, 128), vm(4, r + 16, 128), vm(2, 4, r + 16, 128), vm(4, 17, r + 16, 128),
           pltpu.VMEM((p, r, 128), jnp.int32), pltpu.VMEM((half, 16, 2, 8, 128), jnp.int32), vm(half, 16, 11, 8, 128),
           vm(4, half, 16, 8, 128), vm(4, p, r, 128)]
        + [vm(3, p + 8, rows, 128), vm(3, 3, rows, 128), vm(3, p + 8, rows, 256),
           vm(p + 8, rows, 256), vm(p + 8, rows, 256), vm(p + 8, rows, 128), vm(rows, 128), vm(1, p1, r1, 128)]
        + [vm(2, 1, p1, 2, 128), vm(3, 2, 1, 2, r1, 128), vm(3, 2, 1, p1, 2, 128), vm(3, 2, 2, 1, 2, 2, 128), vm(2, 1, p1, r1, 128)]
        + [vm(3, 1, p1 + 8, rows1, 128), vm(p1 + 8, rows1, 256), vm(p1 + 8, rows1, 256),
           vm(p1 + 8, rows1, 128), vm(rows1, 128), vm(p2, r2, 128), vm(3, 3, 3, p2, r2, 128), vm(3, 3 * p2, 16, 128),
           vm(3 * p2, 2, rows1, 128), vm(p1 + 8, 2, rows, 128)]
        + [dma(34), dma(13), vm(1, 1, r + 16, 128), vm(1, 4, r, 128), vm(1, 4, 8, 128), vm(1, 8, 4, 128), vm(1, 8, 2, 128), vm(512, 128)]
    )
    for hx, hy in ((3, 2), (2, 4), (2, 2)):
        scratch += xy(1, p, r, hx, hy) + [vm(r, 128), vm(2, hy, 128), vm(2, 3, r, 128), vm(2, 3, 2, hy, 128)]
    vmem = pl.BlockSpec(memory_space=pltpu.VMEM)
    results = pl.pallas_call(
        functools.partial(kernel, sizes),
        out_shape=(
            jax.ShapeDtypeStruct(velocity.shape, f32),
            jax.ShapeDtypeStruct(density.shape, f32),
            jax.ShapeDtypeStruct(density.shape, f32),
        ),
        in_specs=[pl.BlockSpec(memory_space=pltpu.HBM)] * 4,
        out_specs=(vmem,) * 3,
        scratch_shapes=scratch,
        compiler_params=pltpu.CompilerParams(
            collective_id=0, has_side_effects=True, vmem_limit_bytes=32 * 1024 * 1024
        ),
    )(*[pltpu.with_memory_space_constraint(a, pltpu.HBM) for a in (velocity, density, offsets, eighths)])
    return write_out(results)


def solution(mesh):
    sizes = tuple(mesh.shape[a] for a in ("gx", "gy", "gz"))
    block = P("gx", "gy", "gz")
    stacked = P(None, "gx", "gy", "gz")
    return jax.shard_map(
        functools.partial(step, sizes),
        mesh=mesh,
        in_specs=(stacked, block, stacked, stacked),
        out_specs=(stacked, block, block),
        check_vma=False,
    )
```
